256 devices in a mesh: seq: 128 (over z, x_hi, y, core), head: 2 (over x_lo).
Axes of the slice: x: 4 (x_hi: 2, x_lo: 2; x = x_hi * 2 + x_lo), y: 4, z: 8, core: 2. Of those that a mesh axis runs over, the one named last changes fastest.
Arguments:
- queries: bfloat16 [32768, 512], P('seq', 'head'), may hold values from -4 to 4
- values: bfloat16 [32768, 512], P('seq', 'head'), may hold values from -6 to 6
- scales: float32 [32768, 8], P('seq', 'head'), may hold values from 2 to 20
- block_reach: int32 [128], P('seq'), may hold values from 1 to 4
- out_weight: bfloat16 [512, 1024], P('head'), may hold values from -0.25 to 0.25
- out_grad: bfloat16 [32768, 512], P('seq', 'head'), may hold values from -6 to 6
Outputs:
- mixed: bfloat16 [32768, 1024], P(('seq', 'head'))
- value_grad: bfloat16 [32768, 512], P('seq', 'head')
The draws below stay inside these ranges and needn't reach their ends.
All inputs are finite; a program needn't handle non-finite values.
Results may differ from the reference program's by a relative error of at most 0.0015.
The reference program's roundings to bfloat16 on the way count: a program that leaves them out, or rounds other values in their place, can miss the bound.
Values may be sent and summed in bfloat16 or wider, within the bound.
A program may use at most 64 MiB of HBM per device.

```python
import math
import jax
import jax.numpy as jnp
from jax import lax

D = 1024
HD = 64
WINDOW = 4
TOK_DEV = 256
HEADS = 8
NBLK = 128
TOKENS = 32768


def query_field(key):
    base_key = jax.random.fold_in(key, 11)
    scale_key = jax.random.fold_in(key, 12)
    logs = jax.random.uniform(scale_key, (TOKENS, HEADS), jnp.float32, math.log(2.0), math.log(20.0))
    spread = jnp.exp(logs)
    raw = jax.random.normal(base_key, (TOKENS, HEADS, HD), jnp.float32)
    return (jnp.clip(raw, -4.0, 4.0), jnp.clip(spread, 2.0, 20.0))


def draw_queries(key, part):
    field = query_field(key)[0]
    return field.reshape(TOKENS, HEADS * HD).astype(jnp.bfloat16)


def draw_scales(key, part):
    return query_field(key)[1]


def plant(values, own_key, smallest, high):
    place = [jax.random.randint(jax.random.fold_in(own_key, axis), (), 0, length) for axis, length in enumerate(values.shape)]
    main_axis = values.shape.index(max(values.shape))
    next_to = place[:main_axis] + [(place[main_axis] + 1) % values.shape[main_axis]] + place[main_axis + 1:]
    return values.at[tuple(place)].set(smallest).at[tuple(next_to)].set(high)


def level_of(stream_key, extent, pieces, least, top_value):
    gain, own = 1.0, jax.random.fold_in(stream_key, 6)
    for axis_at, shards_of in pieces:
        draws = jnp.exp(jax.random.uniform(jax.random.fold_in(own, axis_at), (shards_of,), jnp.float32, least / len(pieces), top_value / len(pieces)))
        gain = gain * jnp.repeat(draws, extent[axis_at] // shards_of).reshape([-1 if axis == axis_at else 1 for axis in range(len(extent))])
    return gain


def noise(own_key, dims, scale, most, pieces=(), held_as=jnp.bfloat16):
    loudness = level_of(own_key, dims, pieces, -0.22, 0.18) if pieces else 1.0
    entries = jax.random.normal(own_key, dims, jnp.float32) * scale * loudness
    return jnp.minimum(jnp.maximum(entries, -most), most).astype(held_as)


def setup_inputs(seed: int = 0) -> dict:
    key_of = jax.random.split(jax.random.key(seed), 7)
    queries = draw_queries(jax.random.fold_in(key_of[6], 71), 0)
    values = noise(key_of[1], (TOKENS, HEADS * HD), 1.0, 6.0, ((0, 128), (1, 2)))
    scales = draw_scales(jax.random.fold_in(key_of[6], 71), 0)
    block_reach = plant(jax.random.randint(key_of[3], (NBLK,), 1, WINDOW + 1), jax.random.fold_in(key_of[3], 1), 1, WINDOW).astype(jnp.int32)
    out_weight = noise(key_of[4], (HEADS * HD, D), (HEADS * HD) ** -0.5, 0.25, ((0, 2),))
    out_grad = noise(key_of[5], (TOKENS, HEADS * HD), 1.0, 6.0, ((0, 128), (1, 2)))
    return dict(queries=queries, values=values, scales=scales, block_reach=block_reach, out_weight=out_weight, out_grad=out_grad)


NEGATIVE = -1e+30

def rounded(tensor):
    return lax.optimization_barrier(tensor.astype(jnp.bfloat16)).astype(jnp.float32)

def unit_keys(queries, scales):
    as_float = queries.astype(jnp.float32).reshape(queries.shape[0], scales.shape[1], HD)
    direction = as_float * lax.rsqrt(lax.optimization_barrier(jnp.sum(as_float * as_float, axis=-1, keepdims=True)) + 1e-06)
    return (direction * scales[:, :, None]).astype(jnp.bfloat16)

def reference(queries, values, scales, block_reach, out_weight, out_grad):
    span = 2 * WINDOW + 1
    key_blocks = rounded(unit_keys(queries, scales)).reshape(NBLK, TOK_DEV, HEADS, HD)
    value_blocks = values.astype(jnp.float32).reshape(NBLK, TOK_DEV, HEADS, HD)
    grad_blocks = out_grad.astype(jnp.float32).reshape(NBLK, TOK_DEV, HEADS, HD)
    padding = jnp.zeros((WINDOW, TOK_DEV, HEADS, HD), jnp.float32)
    padded_keys = jnp.concatenate([padding, key_blocks, padding], axis=0)
    padded_values = jnp.concatenate([padding, value_blocks, padding], axis=0)
    padded_grads = jnp.concatenate([padding, grad_blocks, padding], axis=0)
    reach_pad = jnp.zeros((WINDOW,), jnp.int32)
    padded_reach = jnp.concatenate([reach_pad, block_reach.astype(jnp.int32), reach_pad], axis=0)
    offsets = jnp.arange(span, dtype=jnp.int32) - WINDOW
    diagonal = jnp.eye(TOK_DEV, dtype=bool)
    self_mask = (offsets == 0)[:, None, None, None] & diagonal[None, None, :, :]

    def allowed_near(block):
        nearby = lax.dynamic_slice_in_dim(padded_reach, block, span)
        limit = jnp.minimum(block_reach[block].astype(jnp.int32), nearby)
        return ((offsets == 0) | (jnp.abs(offsets) <= limit)).astype(jnp.float32)

    def forward_block(block):
        own_keys = key_blocks[block]
        near_keys = lax.dynamic_slice_in_dim(padded_keys, block, span, 0)
        near_values = lax.dynamic_slice_in_dim(padded_values, block, span, 0)
        scores = jnp.einsum('ihd,cjhd->chij', own_keys, near_keys)
        scores = jnp.where(self_mask, NEGATIVE, scores)
        allowed = allowed_near(block)[:, None, None]
        tile_top = lax.optimization_barrier(jnp.max(scores, axis=-1))
        exponent = jnp.exp(scores - tile_top[..., None]) * allowed[..., None]
        tile_sums = lax.optimization_barrier(jnp.sum(exponent, axis=-1))
        numerators = jnp.einsum('chij,cjhd->cihd', rounded(exponent), near_values)
        tile_top = jnp.where(allowed > 0, tile_top, NEGATIVE)
        row_top = lax.optimization_barrier(jnp.max(tile_top, axis=0))
        factors = jnp.exp(tile_top - row_top[None])
        totals = lax.optimization_barrier(jnp.sum(factors * tile_sums, axis=0))
        combined = lax.optimization_barrier(jnp.sum(jnp.transpose(factors, (0, 2, 1))[..., None] * numerators, axis=0))
        attended = (combined / jnp.transpose(totals)[:, :, None]).astype(jnp.bfloat16)
        return (attended, row_top, totals)
    attended, row_top, totals = lax.map(forward_block, jnp.arange(NBLK, dtype=jnp.int32))
    flat = attended.reshape(TOKENS, HEADS * HD)
    mixed = jnp.dot(flat, out_weight, preferred_element_type=jnp.float32).astype(jnp.bfloat16)
    padded_top = jnp.concatenate([jnp.zeros((WINDOW, HEADS, TOK_DEV), jnp.float32), row_top, jnp.zeros((WINDOW, HEADS, TOK_DEV), jnp.float32)], axis=0)
    padded_total = jnp.concatenate([jnp.ones((WINDOW, HEADS, TOK_DEV), jnp.float32), totals, jnp.ones((WINDOW, HEADS, TOK_DEV), jnp.float32)], axis=0)

    def grad_block(block):
        own_keys = key_blocks[block]
        near_keys = lax.dynamic_slice_in_dim(padded_keys, block, span, 0)
        near_grads = lax.dynamic_slice_in_dim(padded_grads, block, span, 0)
        near_top = lax.dynamic_slice_in_dim(padded_top, block, span, 0)
        near_total = lax.dynamic_slice_in_dim(padded_total, block, span, 0)
        scores = jnp.einsum('bihd,jhd->bhij', near_keys, own_keys)
        scores = jnp.where(self_mask, NEGATIVE, scores)
        allowed = allowed_near(block)[:, None, None, None]
        weights = jnp.where(allowed > 0, jnp.exp(scores - near_top[..., None]) / near_total[..., None], 0.0)
        return jnp.einsum('bhij,bihd->jhd', rounded(weights), near_grads).astype(jnp.bfloat16)
    value_grad = lax.map(grad_block, jnp.arange(NBLK, dtype=jnp.int32)).reshape(TOKENS, HEADS * HD)
    return (mixed, value_grad)
```

```python
import jax
import jax.numpy as jnp
from jax import lax
from jax.experimental import pallas as pl
from jax.experimental.pallas import tpu as pltpu
from jax.sharding import PartitionSpec as P

HD = 64
TOK = 256
HEADS_DEV = 4
D = 1024
RINGS = 16
RING = 8
NBLK = 128
ROWS = 3 * HD + 16
MESH = pl.DeviceIdType.MESH
START = -1e30
NEGATIVE = -1e30
BARRED = -3e30


def kernel(
    q_ref,
    v_ref,
    g_ref,
    scale_ref,
    reach_ref,
    w_ref,
    mixed_ref,
    vgrad_ref,
    send,
    buf,
    kf,
    kb,
    kta,
    top,
    tot,
    acc,
    lse,
    att,
    att_recv,
    vg,
    vg_recv,
    w_other,
    slot_sem,
    send_sem,
    lse_sem,
    lse_send_sem,
    att_sem,
    att_send_sem,
    vg_sem,
    vg_send_sem,
    w_sem,
    w_send_sem,
):
    me = lax.axis_index("seq")
    grp = lax.axis_index("head")
    ring = me // RING
    inner = me % RING
    y = inner // 2
    k = inner % 2
    other = 1 - grp
    home = y // 2
    partner = me + 1 - 2 * k
    prev_ring = ((ring + RINGS - 1) % RINGS) * RING
    next_ring = ((ring + 1) % RINGS) * RING
    up = y // 2

    halo_from = prev_ring * (1 - k) + next_ring * k + 4 * (1 - k)
    lse_peer = (prev_ring + 2 * y + 1) * (1 - k) + (next_ring + 2 * y) * k
    halo_to = (next_ring) * up + (prev_ring + 1) * (1 - up)
    halo_slot = (2 * y + k - 4) * up + (2 * y + k + 8) * (1 - up)
    own_slot = 2 * y + 4 - 3 * k
    partner_slot = 2 * y + 5 * k
    is_home = (home == k).astype(jnp.int32)

    barrier = pltpu.get_barrier_semaphore()

    def greet(seq, head):
        pl.semaphore_signal(barrier, inc=1, device_id=(seq, head), device_id_type=MESH)

    greet(partner, grp)
    for step in range(1, 4):
        greet(ring * RING + 2 * ((y + step) % 4) + k, grp)
    for j in range(4):
        greet(halo_from + j, grp)
    greet(lse_peer, grp)
    for h in range(4):
        source = ring * RING + 2 * h + home
        greet(source, other)

        @pl.when(jnp.logical_not(source == me))
        def _():
            greet(source, grp)

    greet(me, other)

    q_t = q_ref[...].T
    v_t = v_ref[...].T
    g_t = g_ref[...].T
    reach_rows = jnp.full((16, TOK), reach_ref[0].astype(jnp.float32)).astype(jnp.bfloat16)
    for h in range(HEADS_DEV):
        part = q_t[h * HD : (h + 1) * HD, :].astype(jnp.float32)
        square = jnp.sum(part * part, axis=0, keepdims=True)
        direction = part * lax.rsqrt(square + 1e-06)
        send[h, 0:HD, :] = (direction * scale_ref[h : h + 1, :]).astype(jnp.bfloat16)
        send[h, HD : 2 * HD, :] = v_t[h * HD : (h + 1) * HD, :]
        send[h, 2 * HD : 3 * HD, :] = g_t[h * HD : (h + 1) * HD, :]
        send[h, 3 * HD :, :] = reach_rows

    pl.semaphore_wait(barrier, 18 - is_home)

    def block_copy(src, slot, sent, seq):
        return pltpu.make_async_remote_copy(
            src_ref=src,
            dst_ref=buf.at[slot],
            send_sem=send_sem.at[sent],
            recv_sem=slot_sem.at[slot],
            device_id=(seq, grp),
            device_id_type=MESH,
        )

    block_copy(send.at[y], partner_slot, 0, partner).start()
    for step in (2, 1, 3):
        target = (y + step) % 4
        block_copy(send.at[target], own_slot, step, ring * RING + 2 * target + k).start()
    for h in range(4):
        block_copy(send.at[h], halo_slot, 4 + h, halo_to + 2 * h).start()
    half = pl.multiple_of(k * 128, 128)
    w_copy = pltpu.make_async_remote_copy(
        src_ref=w_ref.at[pl.ds(half, 128)],
        dst_ref=w_other.at[pl.ds(half, 128)],
        send_sem=w_send_sem.at[0],
        recv_sem=w_sem.at[0],
        device_id=(me, other),
        device_id_type=MESH,
    )
    w_copy.start()
    buf[own_slot] = send[y]

    def arrived(slot):
        block_copy(send.at[0], slot, 0, partner).wait_recv()

    for step in (1, 3, 2):
        source = (y + step) % 4
        slot = 2 * source + 4 - 3 * k
        arrived(slot)
        block_copy(buf.at[slot], 2 * source + 5 * k, 7 + step, partner).start()
    for source in range(4):
        arrived(2 * source + 5 - 5 * k)

    def turn(slot):
        kf[slot] = buf[slot, 0:HD, :].T

    def turn_ring(i, carry):
        turn(i + 4 * (1 - k))
        return carry

    lax.fori_loop(0, 8, turn_ring, 0)

    for b in range(4):
        top[b] = jnp.full((1, TOK), START, jnp.float32)
        tot[b] = jnp.zeros((1, TOK), jnp.float32)
        acc[b] = jnp.zeros((HD, TOK), jnp.float32)

    first_block = ring * RING + 4 * k - 4

    def allowed_row(slot, b, distance):
        index = first_block + slot
        valid = jnp.logical_and(index >= 0, index < NBLK)
        needed = jnp.where(valid, distance, 99).astype(jnp.float32)
        far = buf[slot, 3 * HD :, :].astype(jnp.float32)[0:1]
        own = buf[4 + b, 3 * HD :, :].astype(jnp.float32)[0:1]
        return needed <= jnp.minimum(far, own)

    def diagonal():
        return lax.broadcasted_iota(jnp.int32, (TOK, TOK), 0) == lax.broadcasted_iota(
            jnp.int32, (TOK, TOK), 1
        )

    def forward_tile(slot, b, distance, own, state):
        scores = jnp.dot(kf[slot], buf[4 + b, 0:HD, :], preferred_element_type=jnp.float32)
        if own:
            scores = jnp.where(diagonal(), NEGATIVE, scores)
        tile_top = jnp.max(scores, axis=0, keepdims=True)
        exponent = jnp.exp(scores - tile_top)
        tile_sum = jnp.sum(exponent, axis=0, keepdims=True)
        numerator = jnp.dot(
            buf[slot, HD : 2 * HD, :],
            exponent.astype(jnp.bfloat16),
            preferred_element_type=jnp.float32,
        )
        if not own:
            tile_top = jnp.where(allowed_row(slot, b, distance), tile_top, BARRED)
        old_top, old_tot, old_acc = state
        new_top = jnp.maximum(old_top, tile_top)
        keep = jnp.exp(old_top - new_top)
        add = jnp.exp(tile_top - new_top)
        return (
            new_top,
            keep * old_tot + add * tile_sum,
            keep * old_acc + add * numerator,
        )

    def load_state(b):
        return top[b], tot[b], acc[b]

    def store_state(b, state):
        top[b], tot[b], acc[b] = state

    def forward_square(i, carry):
        for step in range(4):
            b = (i + step) % 4
            gap = jnp.abs(i - b)
            store_state(b, forward_tile(4 + i, b, gap, step == 0, load_state(b)))
        return carry

    lax.fori_loop(0, 4, forward_square, 0)

    def corner(right, m, q):
        slot = (8 + m) * right + (3 - m) * (1 - right)
        b = q * right + (3 - q) * (1 - right)
        return slot, b

    def forward_side(phase, carry):
        right = jnp.where(phase == 0, 1 - k, k)

        @pl.when(phase == 1)
        def _():
            for m in range(4):
                slot, _ = corner(right, m, 0)
                arrived(slot)
                turn(slot)

        for q in range(4):
            b = q * right + (3 - q) * (1 - right)
            state = load_state(b)
            for m in range(q + 1):
                slot, _ = corner(right, m, q)
                state = forward_tile(slot, b, 4 + m - q, False, state)
            store_state(b, state)
        return carry

    lax.fori_loop(0, 2, forward_side, 0)

    denominators = [top[b] + jnp.log(tot[b]) for b in range(4)]
    lse[1] = jnp.concatenate(denominators + denominators, axis=0)
    for b in range(4):
        att[b] = (acc[b] * (1.0 / tot[b])).astype(jnp.bfloat16)

    def lse_copy(which, place, seq):
        return pltpu.make_async_remote_copy(
            src_ref=lse.at[1],
            dst_ref=lse.at[place],
            send_sem=lse_send_sem.at[which],
            recv_sem=lse_sem.at[place],
            device_id=(seq, grp),
            device_id_type=MESH,
        )

    lse_copy(0, 2 * k, partner).start()
    lse_copy(1, 2 * (1 - k), lse_peer).start()

    def att_copy(b, head):
        return pltpu.make_async_remote_copy(
            src_ref=att.at[b, :, pl.ds(pl.multiple_of(head * 128, 128), 128)],
            dst_ref=att_recv.at[grp * 4 + y],
            send_sem=att_send_sem.at[b, head],
            recv_sem=att_sem.at[grp * 4 + y],
            device_id=(ring * RING + 4 * k + b, head),
            device_id_type=MESH,
        )

    def owner(b):
        return ring * RING + 4 * k + b

    for b in range(4):
        att_copy(b, other).start()

        @pl.when(jnp.logical_not(owner(b) == me))
        def _():
            att_copy(b, grp).start()

    @pl.when(home == k)
    def _():
        b = inner - 4 * k
        att_recv[grp * 4 + y] = att[b, :, pl.ds(pl.multiple_of(grp * 128, 128), 128)]

    w_copy.wait_recv()
    pltpu.make_async_remote_copy(
        src_ref=w_other.at[pl.ds(half, 128)],
        dst_ref=w_other.at[pl.ds(half, 128)],
        send_sem=w_send_sem.at[1],
        recv_sem=w_sem.at[1],
        device_id=(partner, grp),
        device_id_type=MESH,
    ).start()

    ones = (lax.broadcasted_iota(jnp.int32, (HD, TOK), 0) < 3).astype(jnp.bfloat16)

    def turn_back(place, row):
        slot = 4 * place + row
        value = -lse[place, pl.ds(row, 1), :]
        high = value.astype(jnp.bfloat16).astype(jnp.float32)
        middle = (value - high).astype(jnp.bfloat16).astype(jnp.float32)
        low = value - high - middle
        index = lax.broadcasted_iota(jnp.int32, (HD, TOK), 0)
        extra = jnp.where(
            index == 0, high, jnp.where(index == 1, middle, jnp.where(index == 2, low, 0.0))
        ).astype(jnp.bfloat16)
        full = jnp.concatenate([buf[slot, 0:HD, :], extra], axis=0)
        kb[slot] = full.T

    for b in range(4):
        kta[b] = jnp.concatenate([buf[4 + b, 0:HD, :], ones], axis=0)
        acc[b] = jnp.zeros((HD, TOK), jnp.float32)

    for row in range(4):
        turn_back(1, row)

    def backward_tile(slot, b, distance, own):
        shifted = jnp.dot(kb[slot], kta[b], preferred_element_type=jnp.float32)
        if own:
            shifted = jnp.where(diagonal(), NEGATIVE, shifted)
        weights = jnp.exp(shifted).astype(jnp.bfloat16)
        part = jnp.dot(
            buf[slot, 2 * HD : 3 * HD, :], weights, preferred_element_type=jnp.float32
        )
        if own:
            return part
        return jnp.where(allowed_row(slot, b, distance), part, 0.0)

    def backward_square(i, carry):
        for step in range(4):
            b = (i + step) % 4
            gap = jnp.abs(i - b)
            acc[b] = acc[b] + backward_tile(4 + i, b, gap, step == 0)
        return carry

    lax.fori_loop(0, 4, backward_square, 0)

    def backward_side(phase, carry):
        right = jnp.where(phase == 0, 1 - k, k)
        place = 2 * right
        lse_copy(0, place, partner).wait_recv()
        for row in range(4):
            turn_back(place, row)
        for q in range(4):
            b = q * right + (3 - q) * (1 - right)
            total = acc[b]
            for m in range(q + 1):
                slot, _ = corner(right, m, q)
                total = total + backward_tile(slot, b, 4 + m - q, False)
            acc[b] = total
        return carry

    lax.fori_loop(0, 2, backward_side, 0)

    for b in range(4):
        vg[b] = acc[b].astype(jnp.bfloat16)

    def vg_copy(b):
        return pltpu.make_async_remote_copy(
            src_ref=vg.at[b],
            dst_ref=vg_recv.at[y],
            send_sem=vg_send_sem.at[b],
            recv_sem=vg_sem.at[y],
            device_id=(owner(b), grp),
            device_id_type=MESH,
        )

    for b in range(4):

        @pl.when(jnp.logical_not(owner(b) == me))
        def _():
            vg_copy(b).start()

    @pl.when(home == k)
    def _():
        vg_recv[y] = vg[inner - 4 * k]

    def att_arrived(place):
        pltpu.make_async_remote_copy(
            src_ref=att.at[0, :, pl.ds(0, 128)],
            dst_ref=att_recv.at[place],
            send_sem=att_send_sem.at[0, 0],
            recv_sem=att_sem.at[place],
            device_id=(me, other),
            device_id_type=MESH,
        ).wait_recv()

    for h in range(4):
        att_arrived(other * 4 + h)

        @pl.when(jnp.logical_not(ring * RING + 2 * h + home == me))
        def _():
            att_arrived(grp * 4 + h)

    pltpu.make_async_remote_copy(
        src_ref=w_other.at[pl.ds(half, 128)],
        dst_ref=w_other.at[pl.ds(half, 128)],
        send_sem=w_send_sem.at[1],
        recv_sem=w_sem.at[1],
        device_id=(partner, grp),
        device_id_type=MESH,
    ).wait_recv()
    mine = att_recv[pl.ds(grp * 4, 4)].reshape(4 * HD, 128).T
    theirs = att_recv[pl.ds(other * 4, 4)].reshape(4 * HD, 128).T
    mixed_ref[...] = (
        jnp.dot(mine, w_ref[...], preferred_element_type=jnp.float32)
        + jnp.dot(theirs, w_other[...], preferred_element_type=jnp.float32)
    ).astype(jnp.bfloat16)

    for h in range(4):

        @pl.when(jnp.logical_not(ring * RING + 2 * h + home == me))
        def _():
            pltpu.make_async_remote_copy(
                src_ref=vg.at[0],
                dst_ref=vg_recv.at[h],
                send_sem=vg_send_sem.at[0],
                recv_sem=vg_sem.at[h],
                device_id=(partner, grp),
                device_id_type=MESH,
            ).wait_recv()

    vgrad_ref[...] = vg_recv[...].reshape(4 * HD, TOK).T

    for sent in range(11):
        block_copy(send.at[0], 0, sent, partner).wait_send()
    w_copy.wait_send()
    pltpu.make_async_remote_copy(
        src_ref=w_other.at[pl.ds(half, 128)],
        dst_ref=w_other.at[pl.ds(half, 128)],
        send_sem=w_send_sem.at[1],
        recv_sem=w_sem.at[1],
        device_id=(partner, grp),
        device_id_type=MESH,
    ).wait_send()
    lse_copy(0, 0, partner).wait_send()
    lse_copy(1, 0, partner).wait_send()
    for b in range(4):
        att_copy(b, other).wait_send()

        @pl.when(jnp.logical_not(owner(b) == me))
        def _():
            att_copy(b, grp).wait_send()
            vg_copy(b).wait_send()


def shards(queries, values, scales, block_reach, out_weight, out_grad):
    vmem = pl.BlockSpec(memory_space=pltpu.VMEM)
    bf16, f32 = jnp.bfloat16, jnp.float32
    dma = pltpu.SemaphoreType.DMA
    return pl.pallas_call(
        kernel,
        out_shape=(
            jax.ShapeDtypeStruct((TOK // 2, D), bf16),
            jax.ShapeDtypeStruct((TOK, HEADS_DEV * HD), bf16),
        ),
        in_specs=[vmem, vmem, vmem, vmem, pl.BlockSpec(memory_space=pltpu.SMEM), vmem],
        out_specs=(vmem, vmem),
        scratch_shapes=[
            pltpu.VMEM((4, ROWS, TOK), bf16),
            pltpu.VMEM((12, ROWS, TOK), bf16),
            pltpu.VMEM((12, TOK, HD), bf16),
            pltpu.VMEM((12, TOK, 2 * HD), bf16),
            pltpu.VMEM((4, 2 * HD, TOK), bf16),
            pltpu.VMEM((4, 1, TOK), f32),
            pltpu.VMEM((4, 1, TOK), f32),
            pltpu.VMEM((4, HD, TOK), f32),
            pltpu.VMEM((3, 8, TOK), f32),
            pltpu.VMEM((4, HD, TOK), bf16),
            pltpu.VMEM((8, HD, TOK // 2), bf16),
            pltpu.VMEM((4, HD, TOK), bf16),
            pltpu.VMEM((4, HD, TOK), bf16),
            pltpu.VMEM((TOK, D), bf16),
            dma((12,)),
            dma((11,)),
            dma((3,)),
            dma((2,)),
            dma((8,)),
            dma((4, 2)),
            dma((4,)),
            dma((4,)),
            dma((2,)),
            dma((2,)),
        ],
        compiler_params=pltpu.CompilerParams(
            collective_id=0, has_side_effects=True, vmem_limit_bytes=48 * 1024 * 1024
        ),
    )(queries, values, out_grad, scales.T, block_reach, out_weight)


def solution(mesh):
    return jax.shard_map(
        shards,
        mesh=mesh,
        in_specs=(
            P("seq", "head"),
            P("seq", "head"),
            P("seq", "head"),
            P("seq"),
            P("head", None),
            P("seq", "head"),
        ),
        out_specs=(P(("seq", "head"), None), P("seq", "head")),
        check_vma=False,
    )
```

```python
import jax
import jax.numpy as jnp
from jax import lax
from jax.experimental import pallas as pl
from jax.experimental.pallas import tpu as pltpu
from jax.sharding import PartitionSpec as P

HD = 64
TOK = 256
HEADS_DEV = 4
D = 1024
RINGS = 16
RING = 8
NBLK = 128
ROWS = 2 * HD + 16
MESH = pl.DeviceIdType.MESH
START = -1e30
NEGATIVE = -1e30
BARRED = -3e30


def kernel(
    q_hbm,
    v_hbm,
    g_hbm,
    scale_hbm,
    reach_ref,
    w_hbm,
    mixed_ref,
    vgrad_ref,
    q_ref,
    v_ref,
    g_ref,
    scale_ref,
    w_ref,
    send,
    send_g,
    buf,
    buf_g,
    kf,
    tiles,
    weights,
    columns,
    top,
    tot,
    acc,
    lse,
    att,
    att_recv,
    vg,
    vg_recv,
    w_other,
    slot_sem,
    send_sem,
    slot_g_sem,
    send_g_sem,
    lse_sem,
    lse_send_sem,
    att_sem,
    att_send_sem,
    vg_sem,
    vg_send_sem,
    w_sem,
    w_send_sem,
    in_sem,
):
    me = lax.axis_index("seq")
    grp = lax.axis_index("head")
    ring = me // RING
    inner = me % RING
    y = inner // 2
    k = inner % 2
    other = 1 - grp
    home = y // 2
    partner = me + 1 - 2 * k
    prev_ring = ((ring + RINGS - 1) % RINGS) * RING
    next_ring = ((ring + 1) % RINGS) * RING
    up = y // 2

    halo_from = prev_ring * (1 - k) + next_ring * k + 4 * (1 - k)
    lse_peer = (prev_ring + 2 * y + 1) * (1 - k) + (next_ring + 2 * y) * k
    halo_to = (next_ring) * up + (prev_ring + 1) * (1 - up)
    halo_slot = (2 * y + k - 4) * up + (2 * y + k + 8) * (1 - up)
    own_slot = 2 * y + 4 - 3 * k
    partner_slot = 2 * y + 5 * k
    is_home = (home == k).astype(jnp.int32)
    first, last = ring == 0, ring == RINGS - 1
    gets = jnp.logical_not(jnp.logical_or(jnp.logical_and(first, k == 0), jnp.logical_and(last, k == 1)))
    gives = jnp.logical_not(jnp.logical_or(jnp.logical_and(first, up == 0), jnp.logical_and(last, up == 1)))
    expected = 13 - is_home + gets.astype(jnp.int32) + 4 * gives.astype(jnp.int32)

    barrier = pltpu.get_barrier_semaphore()
    loads = [
        pltpu.make_async_copy(source, target, in_sem.at[i])
        for i, (source, target) in enumerate(
            (
                (q_hbm, q_ref),
                (scale_hbm, scale_ref),
                (v_hbm, v_ref),
                (g_hbm, g_ref),
                (w_hbm, w_ref),
            )
        )
    ]
    for load in loads:
        load.start()

    def greet(seq, head):
        pl.semaphore_signal(barrier, inc=1, device_id=(seq, head), device_id_type=MESH)

    greet(partner, grp)
    for step in range(1, 4):
        greet(ring * RING + 2 * ((y + step) % 4) + k, grp)

    @pl.when(gets)
    def _():
        for j in range(4):
            greet(halo_from + j, grp)
        greet(lse_peer, grp)

    for h in range(4):
        source = ring * RING + 2 * h + home
        greet(source, other)

        @pl.when(jnp.logical_not(source == me))
        def _():
            greet(source, grp)

    greet(me, other)

    for load in loads[:4]:
        load.wait()
    q_t = q_ref[...].T
    v_t = v_ref[...].T
    g_t = g_ref[...].T
    reach_rows = jnp.full((16, TOK), reach_ref[0].astype(jnp.float32)).astype(jnp.bfloat16)
    for h in range(HEADS_DEV):
        part = q_t[h * HD : (h + 1) * HD, :].astype(jnp.float32)
        square = jnp.sum(part * part, axis=0, keepdims=True)
        direction = part * lax.rsqrt(square + 1e-06)
        send[h, 0:HD, :] = (direction * scale_ref[h : h + 1, :]).astype(jnp.bfloat16)
        send[h, HD : 2 * HD, :] = v_t[h * HD : (h + 1) * HD, :]
        send[h, 2 * HD :, :] = reach_rows
        send_g[h] = g_t[h * HD : (h + 1) * HD, :]

    pl.semaphore_wait(barrier, expected)

    def block_copy(src, slot, sent, seq):
        return pltpu.make_async_remote_copy(
            src_ref=src,
            dst_ref=buf.at[slot],
            send_sem=send_sem.at[sent],
            recv_sem=slot_sem.at[slot],
            device_id=(seq, grp),
            device_id_type=MESH,
        )

    def grad_copy(src, slot, sent, seq):
        return pltpu.make_async_remote_copy(
            src_ref=src,
            dst_ref=buf_g.at[slot],
            send_sem=send_g_sem.at[sent],
            recv_sem=slot_g_sem.at[slot],
            device_id=(seq, grp),
            device_id_type=MESH,
        )

    for step in (2, 1, 3):
        target = (y + step) % 4
        block_copy(send.at[target], own_slot, step, ring * RING + 2 * target + k).start()
    block_copy(send.at[y], partner_slot, 0, partner).start()

    @pl.when(gives)
    def _():
        for step in (0, 1, 3, 2):
            target = (y + step) % 4
            block_copy(send.at[target], halo_slot, 4 + step, halo_to + 2 * target).start()

    for step in (2, 1, 3):
        target = (y + step) % 4
        grad_copy(send_g.at[target], own_slot, step, ring * RING + 2 * target + k).start()
    grad_copy(send_g.at[y], partner_slot, 0, partner).start()

    @pl.when(gives)
    def _():
        for step in (0, 1, 3, 2):
            target = (y + step) % 4
            grad_copy(send_g.at[target], halo_slot, 4 + step, halo_to + 2 * target).start()

    half = pl.multiple_of(k * 128, 128)
    w_copy = pltpu.make_async_remote_copy(
        src_ref=w_hbm.at[pl.ds(half, 128)],
        dst_ref=w_other.at[pl.ds(half, 128)],
        send_sem=w_send_sem.at[0],
        recv_sem=w_sem.at[0],
        device_id=(me, other),
        device_id_type=MESH,
    )
    w_copy.start()
    buf[own_slot] = send[y]
    buf_g[own_slot] = send_g[y]

    @pl.when(jnp.logical_not(gets))
    def _():
        for m in range(4):
            slot = (8 + m) * k + m * (1 - k)
            buf[slot] = jnp.zeros((ROWS, TOK), jnp.bfloat16)
            buf_g[slot] = jnp.zeros((HD, TOK), jnp.bfloat16)
        lse[2 * k] = jnp.zeros((8, TOK), jnp.float32)

    def arrived(slot):
        block_copy(send.at[0], slot, 0, partner).wait_recv()

    def grad_arrived(slot):
        grad_copy(send_g.at[0], slot, 0, partner).wait_recv()

    for step in (1, 3, 2):
        source = (y + step) % 4
        slot = 2 * source + 4 - 3 * k
        arrived(slot)
        block_copy(buf.at[slot], 2 * source + 5 * k, 7 + step, partner).start()
    for source in range(4):
        arrived(2 * source + 5 - 5 * k)

    def turn(slot):
        kf[slot] = buf[slot, 0:HD, :].T

    first_block = ring * RING + 4 * k - 4

    def allowed_row(slot, b, distance):
        index = first_block + slot
        valid = jnp.logical_and(index >= 0, index < NBLK)
        needed = jnp.where(valid, distance, 99).astype(jnp.float32)
        far = buf[slot, 2 * HD :, :].astype(jnp.float32)[0:1]
        mine = buf[4 + b, 2 * HD :, :].astype(jnp.float32)[0:1]
        return needed <= jnp.minimum(far, mine)

    def score_tile(tile):
        slot, b, place, distance = tile
        scores = jnp.dot(kf[slot], buf[4 + b, 0:HD, :], preferred_element_type=jnp.float32)
        if distance is None:
            row = lax.broadcasted_iota(jnp.int32, (TOK, TOK), 0)
            column = lax.broadcasted_iota(jnp.int32, (TOK, TOK), 1)
            scores = jnp.where(row == column, NEGATIVE, scores)
        tiles[place] = scores

    def exponent_tile(tile, spot):
        scores = tiles[tile[2]]
        tile_top = jnp.max(scores, axis=0, keepdims=True)
        exponent = jnp.exp(scores - tile_top)
        weights[spot] = exponent.astype(jnp.bfloat16)
        return tile_top, jnp.sum(exponent, axis=0, keepdims=True)

    def merge_tile(tile, spot, tile_top, tile_sum):
        slot, b, _, distance = tile
        numerator = jnp.dot(
            buf[slot, HD : 2 * HD, :], weights[spot], preferred_element_type=jnp.float32
        )
        if distance is None:
            top[b], tot[b], acc[b] = tile_top, tile_sum, numerator
            return
        tile_top = jnp.where(allowed_row(slot, b, distance), tile_top, BARRED)
        new_top = jnp.maximum(top[b], tile_top)
        keep = jnp.exp(top[b] - new_top)
        add = jnp.exp(tile_top - new_top)
        top[b] = new_top
        tot[b] = keep * tot[b] + add * tile_sum
        acc[b] = keep * acc[b] + add * numerator

    def forward(work):
        count = len(work)
        stats = [None] * count
        for t in range(count + 3):
            if 2 <= t < count + 2:
                stats[t - 2] = exponent_tile(work[t - 2], (t - 2) % 4)
            if t < count:
                score_tile(work[t])
            if t >= 3:
                merge_tile(work[t - 3], (t - 3) % 4, *stats[t - 3])

    square = [
        (4 + i, (i + step) % 4, 9 * ((i + step) % 4) + 4 + i - (i + step) % 4, abs(i - (i + step) % 4) or None)
        for step in range(4)
        for i in range(4)
    ]

    def side(right):
        work = []
        for q in range(4):
            for m in range(q + 1):
                slot = (8 + m) * right + (3 - m) * (1 - right)
                b = q * right + (3 - q) * (1 - right)
                work.append((slot, b, 9 * b + slot - b, 4 + m - q))
        return work

    near, far = 1 - k, k

    for i in range(8):
        turn(i + 4 * near)
    forward(square + side(near))
    for step in (1, 3, 2):
        source = (y + step) % 4
        slot = 2 * source + 4 - 3 * k
        grad_arrived(slot)
        grad_copy(buf_g.at[slot], 2 * source + 5 * k, 7 + step, partner).start()
    @pl.when(gets)
    def _():
        for m in range(4):
            arrived((8 + m) * far + (3 - m) * (1 - far))

    for m in range(4):
        turn((8 + m) * far + (3 - m) * (1 - far))
    forward(side(far))

    denominators = [top[b] + jnp.log(tot[b]) for b in range(4)]
    lse[1] = jnp.concatenate(denominators + denominators, axis=0)
    for b in range(4):
        att[b] = (acc[b] * (1.0 / tot[b])).astype(jnp.bfloat16)

    def lse_copy(which, place, seq):
        return pltpu.make_async_remote_copy(
            src_ref=lse.at[1],
            dst_ref=lse.at[place],
            send_sem=lse_send_sem.at[which],
            recv_sem=lse_sem.at[place],
            device_id=(seq, grp),
            device_id_type=MESH,
        )

    @pl.when(gets)
    def _():
        lse_copy(1, 2 * (1 - k), lse_peer).start()

    lse_copy(0, 2 * k, partner).start()

    def att_copy(b, head):
        return pltpu.make_async_remote_copy(
            src_ref=att.at[b, :, pl.ds(pl.multiple_of(head * 128, 128), 128)],
            dst_ref=att_recv.at[grp * 4 + y],
            send_sem=att_send_sem.at[b, head],
            recv_sem=att_sem.at[grp * 4 + y],
            device_id=(ring * RING + 4 * k + b, head),
            device_id_type=MESH,
        )

    def owner(b):
        return ring * RING + 4 * k + b

    for b in range(4):
        att_copy(b, other).start()

        @pl.when(jnp.logical_not(owner(b) == me))
        def _():
            att_copy(b, grp).start()

    @pl.when(home == k)
    def _():
        b = inner - 4 * k
        att_recv[grp * 4 + y] = att[b, :, pl.ds(pl.multiple_of(grp * 128, 128), 128)]

    def turn_lse(place):
        for row in range(4):
            value = jnp.broadcast_to(lse[place, pl.ds(row, 1), :], (128, TOK))
            columns[4 * place + row] = value.T

    def backward_tile(tile):
        slot, b, place, distance = tile
        column = columns[slot]
        shifted = tiles[place] - jnp.concatenate([column, column], axis=1)
        share = jnp.exp(shifted).astype(jnp.bfloat16)
        part = jnp.dot(buf_g[slot], share, preferred_element_type=jnp.float32)
        if distance is None:
            return part
        return jnp.where(allowed_row(slot, b, distance), part, 0.0)

    for step in range(4):
        grad_arrived(2 * step + 5 - 5 * k)
    turn_lse(1)
    for b in range(4):
        total = None
        for tile in square:
            if tile[1] == b:
                part = backward_tile(tile)
                total = part if total is None else total + part
        acc[b] = total

    def backward_side(right):
        work = side(right)
        for q in range(4):
            first = q * (q + 1) // 2
            b = work[first][1]
            total = acc[b]
            for tile in work[first : first + q + 1]:
                total = total + backward_tile(tile)
            acc[b] = total

    lse_copy(0, 2 * near, partner).wait_recv()
    turn_lse(2 * near)
    backward_side(near)
    @pl.when(gets)
    def _():
        lse_copy(0, 2 * far, partner).wait_recv()
        for m in range(4):
            grad_arrived((8 + m) * far + (3 - m) * (1 - far))

    turn_lse(2 * far)
    backward_side(far)

    for b in range(4):
        vg[b] = acc[b].astype(jnp.bfloat16)

    def vg_copy(b):
        return pltpu.make_async_remote_copy(
            src_ref=vg.at[b],
            dst_ref=vg_recv.at[y],
            send_sem=vg_send_sem.at[b],
            recv_sem=vg_sem.at[y],
            device_id=(owner(b), grp),
            device_id_type=MESH,
        )

    for b in range(4):

        @pl.when(jnp.logical_not(owner(b) == me))
        def _():
            vg_copy(b).start()

    @pl.when(home == k)
    def _():
        vg_recv[y] = vg[inner - 4 * k]

    w_copy.wait_recv()
    pltpu.make_async_remote_copy(
        src_ref=w_other.at[pl.ds(half, 128)],
        dst_ref=w_other.at[pl.ds(half, 128)],
        send_sem=w_send_sem.at[1],
        recv_sem=w_sem.at[1],
        device_id=(partner, grp),
        device_id_type=MESH,
    ).start()

    def att_arrived(place):
        pltpu.make_async_remote_copy(
            src_ref=att.at[0, :, pl.ds(0, 128)],
            dst_ref=att_recv.at[place],
            send_sem=att_send_sem.at[0, 0],
            recv_sem=att_sem.at[place],
            device_id=(me, other),
            device_id_type=MESH,
        ).wait_recv()

    for h in range(4):
        att_arrived(other * 4 + h)

        @pl.when(jnp.logical_not(ring * RING + 2 * h + home == me))
        def _():
            att_arrived(grp * 4 + h)

    pltpu.make_async_remote_copy(
        src_ref=w_other.at[pl.ds(half, 128)],
        dst_ref=w_other.at[pl.ds(half, 128)],
        send_sem=w_send_sem.at[1],
        recv_sem=w_sem.at[1],
        device_id=(partner, grp),
        device_id_type=MESH,
    ).wait_recv()
    loads[4].wait()
    mine = att_recv[pl.ds(grp * 4, 4)].reshape(4 * HD, 128).T
    theirs = att_recv[pl.ds(other * 4, 4)].reshape(4 * HD, 128).T
    mixed_ref[...] = (
        jnp.dot(mine, w_ref[...], preferred_element_type=jnp.float32)
        + jnp.dot(theirs, w_other[...], preferred_element_type=jnp.float32)
    ).astype(jnp.bfloat16)

    for h in range(4):

        @pl.when(jnp.logical_not(ring * RING + 2 * h + home == me))
        def _():
            pltpu.make_async_remote_copy(
                src_ref=vg.at[0],
                dst_ref=vg_recv.at[h],
                send_sem=vg_send_sem.at[0],
                recv_sem=vg_sem.at[h],
                device_id=(partner, grp),
                device_id_type=MESH,
            ).wait_recv()

    vgrad_ref[...] = vg_recv[...].reshape(4 * HD, TOK).T

    for sent in (0, 1, 2, 3, 8, 9, 10):
        block_copy(send.at[0], 0, sent, partner).wait_send()
        grad_copy(send_g.at[0], 0, sent, partner).wait_send()

    @pl.when(gives)
    def _():
        for sent in range(4, 8):
            block_copy(send.at[0], 0, sent, partner).wait_send()
            grad_copy(send_g.at[0], 0, sent, partner).wait_send()

    w_copy.wait_send()
    pltpu.make_async_remote_copy(
        src_ref=w_other.at[pl.ds(half, 128)],
        dst_ref=w_other.at[pl.ds(half, 128)],
        send_sem=w_send_sem.at[1],
        recv_sem=w_sem.at[1],
        device_id=(partner, grp),
        device_id_type=MESH,
    ).wait_send()
    lse_copy(0, 0, partner).wait_send()

    @pl.when(gets)
    def _():
        lse_copy(1, 0, partner).wait_send()

    for b in range(4):
        att_copy(b, other).wait_send()

        @pl.when(jnp.logical_not(owner(b) == me))
        def _():
            att_copy(b, grp).wait_send()
            vg_copy(b).wait_send()


def shards(queries, values, scales, block_reach, out_weight, out_grad):
    vmem = pl.BlockSpec(memory_space=pltpu.VMEM)
    hbm = pl.BlockSpec(memory_space=pltpu.HBM)
    bf16, f32 = jnp.bfloat16, jnp.float32
    dma = pltpu.SemaphoreType.DMA
    return pl.pallas_call(
        kernel,
        out_shape=(
            jax.ShapeDtypeStruct((TOK // 2, D), bf16),
            jax.ShapeDtypeStruct((TOK, HEADS_DEV * HD), bf16),
        ),
        in_specs=[hbm, hbm, hbm, hbm, pl.BlockSpec(memory_space=pltpu.SMEM), hbm],
        out_specs=(vmem, vmem),
        scratch_shapes=[
            pltpu.VMEM((TOK, HEADS_DEV * HD), bf16),
            pltpu.VMEM((TOK, HEADS_DEV * HD), bf16),
            pltpu.VMEM((TOK, HEADS_DEV * HD), bf16),
            pltpu.VMEM((HEADS_DEV, TOK), f32),
            pltpu.VMEM((HEADS_DEV * HD, D), bf16),
            pltpu.VMEM((4, ROWS, TOK), bf16),
            pltpu.VMEM((4, HD, TOK), bf16),
            pltpu.VMEM((12, ROWS, TOK), bf16),
            pltpu.VMEM((12, HD, TOK), bf16),
            pltpu.VMEM((12, TOK, HD), bf16),
            pltpu.VMEM((36, TOK, TOK), f32),
            pltpu.VMEM((4, TOK, TOK), bf16),
            pltpu.VMEM((12, TOK, 128), f32),
            pltpu.VMEM((4, 1, TOK), f32),
            pltpu.VMEM((4, 1, TOK), f32),
            pltpu.VMEM((4, HD, TOK), f32),
            pltpu.VMEM((3, 8, TOK), f32),
            pltpu.VMEM((4, HD, TOK), bf16),
            pltpu.VMEM((8, HD, TOK // 2), bf16),
            pltpu.VMEM((4, HD, TOK), bf16),
            pltpu.VMEM((4, HD, TOK), bf16),
            pltpu.VMEM((TOK, D), bf16),
            dma((12,)),
            dma((11,)),
            dma((12,)),
            dma((11,)),
            dma((3,)),
            dma((2,)),
            dma((8,)),
            dma((4, 2)),
            dma((4,)),
            dma((4,)),
            dma((2,)),
            dma((2,)),
            dma((5,)),
        ],
        compiler_params=pltpu.CompilerParams(
            collective_id=0, has_side_effects=True, vmem_limit_bytes=62 * 1024 * 1024
        ),
    )(queries, values, out_grad, scales.T, block_reach, out_weight)


def solution(mesh):
    return jax.shard_map(
        shards,
        mesh=mesh,
        in_specs=(
            P("seq", "head"),
            P("seq", "head"),
            P("seq", "head"),
            P("seq"),
            P("head", None),
            P("seq", "head"),
        ),
        out_specs=(P(("seq", "head"), None), P("seq", "head")),
        check_vma=False,
    )
```

```python
import jax
import jax.numpy as jnp
from jax import lax
from jax.experimental import pallas as pl
from jax.experimental.pallas import tpu as pltpu
from jax.sharding import PartitionSpec as P

HD = 64
TOK = 256
HEADS_DEV = 4
D = 1024
RINGS = 16
RING = 8
NBLK = 128
ROWS = 2 * HD + 16
HALF = TOK // 2
MESH = pl.DeviceIdType.MESH
START = -1e30
NEGATIVE = -1e30
BARRED = -3e30


def kernel(
    q_hbm,
    v_hbm,
    g_hbm,
    scale_hbm,
    reach_ref,
    w_hbm,
    mixed_ref,
    vgrad_ref,
    q_ref,
    v_ref,
    g_ref,
    scale_ref,
    w_ref,
    send,
    send_v,
    send_g,
    buf,
    buf_v,
    buf_g,
    kf,
    tiles,
    weights,
    columns,
    tile_tops,
    top,
    tot,
    acc,
    lse,
    att,
    att_recv,
    vg,
    vg_recv,
    w_other,
    slot_sem,
    send_sem,
    slot_v_sem,
    send_v_sem,
    slot_g_sem,
    send_g_sem,
    lse_sem,
    lse_send_sem,
    att_sem,
    att_send_sem,
    vg_sem,
    vg_send_sem,
    w_sem,
    w_send_sem,
    in_sem,
):
    me = lax.axis_index("seq")
    grp = lax.axis_index("head")
    ring = me // RING
    inner = me % RING
    y = inner // 2
    k = inner % 2
    other = 1 - grp
    home = y // 2
    partner = me + 1 - 2 * k
    prev_ring = ((ring + RINGS - 1) % RINGS) * RING
    next_ring = ((ring + 1) % RINGS) * RING
    up = y // 2
    across = me + RING - 2 * RING * (ring % 2)

    halo_from = prev_ring * (1 - k) + next_ring * k + 4 * (1 - k)
    lse_peer = (prev_ring + 2 * y + 1) * (1 - k) + (next_ring + 2 * y) * k
    halo_to = (next_ring) * up + (prev_ring + 1) * (1 - up)
    halo_slot = (2 * y + k - 4) * up + (2 * y + k + 8) * (1 - up)
    own_slot = 2 * y + 4 - 3 * k
    partner_slot = 2 * y + 5 * k
    is_home = (home == k).astype(jnp.int32)
    first, last = ring == 0, ring == RINGS - 1
    gets = jnp.logical_not(jnp.logical_or(jnp.logical_and(first, k == 0), jnp.logical_and(last, k == 1)))
    gives = jnp.logical_not(jnp.logical_or(jnp.logical_and(first, up == 0), jnp.logical_and(last, up == 1)))
    expected = 14 - is_home + gets.astype(jnp.int32) + 4 * gives.astype(jnp.int32)

    barrier = pltpu.get_barrier_semaphore()
    loads = [
        pltpu.make_async_copy(source, target, in_sem.at[i])
        for i, (source, target) in enumerate(
            (
                (q_hbm, q_ref),
                (scale_hbm, scale_ref),
                (v_hbm, v_ref),
                (g_hbm, g_ref),
                (w_hbm, w_ref),
            )
        )
    ]
    for load in loads:
        load.start()

    def greet(seq, head):
        pl.semaphore_signal(barrier, inc=1, device_id=(seq, head), device_id_type=MESH)

    greet(partner, grp)
    for step in range(1, 4):
        greet(ring * RING + 2 * ((y + step) % 4) + k, grp)

    @pl.when(gets)
    def _():
        for j in range(4):
            greet(halo_from + j, grp)
        greet(lse_peer, grp)

    for h in range(4):
        source = ring * RING + 2 * h + home
        greet(source, other)

        @pl.when(jnp.logical_not(source == me))
        def _():
            greet(source, grp)

    greet(me, other)
    greet(across, other)

    for load in loads[:4]:
        load.wait()
    q_t = q_ref[...].T
    v_t = v_ref[...].T
    g_t = g_ref[...].T
    reach_rows = jnp.full((16, HALF), reach_ref[0].astype(jnp.float32)).astype(jnp.bfloat16)
    for h in range(HEADS_DEV):
        part = q_t[h * HD : (h + 1) * HD, :].astype(jnp.float32)
        square = jnp.sum(part * part, axis=0, keepdims=True)
        direction = part * lax.rsqrt(square + 1e-06)
        key = (direction * scale_ref[h : h + 1, :]).astype(jnp.bfloat16)
        send[h, 0:HD, :] = key[:, 0:HALF]
        send[h, HD : 2 * HD, :] = key[:, HALF:]
        send[h, 2 * HD :, :] = reach_rows
        send_v[h] = v_t[h * HD : (h + 1) * HD, :]
        send_g[h] = g_t[h * HD : (h + 1) * HD, :]

    pl.semaphore_wait(barrier, expected)

    class Stream:
        def __init__(self, source, place, arrive, sent):
            self.source, self.place, self.arrive, self.sent = source, place, arrive, sent

        def copy(self, src, slot, which, seq):
            return pltpu.make_async_remote_copy(
                src_ref=src,
                dst_ref=self.place.at[slot],
                send_sem=self.sent.at[which],
                recv_sem=self.arrive.at[slot],
                device_id=(seq, grp),
                device_id_type=MESH,
            )

        def start(self):
            for step in (2, 1, 3):
                target = (y + step) % 4
                self.copy(
                    self.source.at[target], own_slot, step, ring * RING + 2 * target + k
                ).start()
            self.copy(self.source.at[y], partner_slot, 0, partner).start()

            @pl.when(gives)
            def _():
                for step in (0, 1, 3, 2):
                    target = (y + step) % 4
                    self.copy(
                        self.source.at[target], halo_slot, 4 + step, halo_to + 2 * target
                    ).start()

        def arrived(self, slot):
            self.copy(self.source.at[0], slot, 0, partner).wait_recv()

        def relay(self):
            for step in (1, 3, 2):
                source = (y + step) % 4
                slot = 2 * source + 4 - 3 * k
                self.arrived(slot)
                self.copy(self.place.at[slot], 2 * source + 5 * k, 7 + step, partner).start()

        def ring_arrived(self):
            for source in range(4):
                self.arrived(2 * source + 5 - 5 * k)

        def halo_arrived(self):
            @pl.when(gets)
            def _():
                for m in range(4):
                    self.arrived((8 + m) * k + (3 - m) * (1 - k))

        def finish(self):
            for which in (0, 1, 2, 3, 8, 9, 10):
                self.copy(self.source.at[0], 0, which, partner).wait_send()

            @pl.when(gives)
            def _():
                for which in range(4, 8):
                    self.copy(self.source.at[0], 0, which, partner).wait_send()

    keys = Stream(send, buf, slot_sem, send_sem)
    vals = Stream(send_v, buf_v, slot_v_sem, send_v_sem)
    grads = Stream(send_g, buf_g, slot_g_sem, send_g_sem)
    for stream in (keys, vals, grads):
        stream.start()
    buf[own_slot] = send[y]
    buf_v[own_slot] = send_v[y]
    buf_g[own_slot] = send_g[y]

    @pl.when(jnp.logical_not(gets))
    def _():
        for m in range(4):
            slot = (8 + m) * k + m * (1 - k)
            buf[slot] = jnp.zeros((ROWS, HALF), jnp.bfloat16)
            buf_v[slot] = jnp.zeros((HD, TOK), jnp.bfloat16)
            buf_g[slot] = jnp.zeros((HD, TOK), jnp.bfloat16)
        lse[2 * k] = jnp.zeros((8, TOK), jnp.float32)

    keys.relay()
    keys.ring_arrived()

    def key_of(slot):
        return jnp.concatenate([buf[slot, 0:HD, :], buf[slot, HD : 2 * HD, :]], axis=1)

    def turn(slot):
        kf[slot] = key_of(slot).T

    first_block = ring * RING + 4 * k - 4

    def allowed_row(slot, b, distance):
        index = first_block + slot
        valid = jnp.logical_and(index >= 0, index < NBLK)
        needed = jnp.where(valid, distance, 99).astype(jnp.float32)
        far = buf[slot, 2 * HD :, :].astype(jnp.float32)[0:1]
        mine = buf[4 + b, 2 * HD :, :].astype(jnp.float32)[0:1]
        row = needed <= jnp.minimum(far, mine)
        return jnp.concatenate([row, row], axis=1)

    def score_tile(tile):
        slot, b, place, distance = tile
        scores = jnp.dot(kf[slot], key_of(4 + b), preferred_element_type=jnp.float32)
        if distance is None:
            row = lax.broadcasted_iota(jnp.int32, (TOK, TOK), 0)
            column = lax.broadcasted_iota(jnp.int32, (TOK, TOK), 1)
            scores = jnp.where(row == column, NEGATIVE, scores)
        tiles[place] = scores

    def exponent_tile(tile):
        slot, b, place, distance = tile
        scores = tiles[place]
        tile_top = jnp.max(scores, axis=0, keepdims=True)
        exponent = jnp.exp(scores - tile_top)
        weights[place] = exponent.astype(jnp.bfloat16)
        tile_sum = jnp.sum(exponent, axis=0, keepdims=True)
        if distance is None:
            tile_tops[place], top[b], tot[b] = tile_top, tile_top, tile_sum
            return
        tile_top = jnp.where(allowed_row(slot, b, distance), tile_top, BARRED)
        new_top = jnp.maximum(top[b], tile_top)
        tile_tops[place] = tile_top
        tot[b] = jnp.exp(top[b] - new_top) * tot[b] + jnp.exp(tile_top - new_top) * tile_sum
        top[b] = new_top

    def exponents(work):
        for t in range(len(work) + 2):
            if t >= 2:
                exponent_tile(work[t - 2])
            if t < len(work):
                score_tile(work[t])

    def numerator_tile(tile):
        slot, b, place, _ = tile
        part = jnp.dot(buf_v[slot], weights[place], preferred_element_type=jnp.float32)
        return jnp.exp(tile_tops[place] - top[b]) * part

    square = [
        (4 + i, (i + step) % 4, 9 * ((i + step) % 4) + 4 + i - (i + step) % 4, abs(i - (i + step) % 4) or None)
        for step in range(4)
        for i in range(4)
    ]

    def side(right):
        work = []
        for q in range(4):
            for m in range(q + 1):
                slot = (8 + m) * right + (3 - m) * (1 - right)
                b = q * right + (3 - q) * (1 - right)
                work.append((slot, b, 9 * b + slot - b, 4 + m - q))
        return work

    near, far = 1 - k, k

    for i in range(8):
        turn(i + 4 * near)
    exponents(square + side(near))
    vals.relay()
    keys.halo_arrived()
    for m in range(4):
        turn((8 + m) * far + (3 - m) * (1 - far))
    exponents(side(far))

    denominators = [top[b] + jnp.log(tot[b]) for b in range(4)]
    lse[1] = jnp.concatenate(denominators + denominators, axis=0)

    def lse_copy(which, place, seq):
        return pltpu.make_async_remote_copy(
            src_ref=lse.at[1],
            dst_ref=lse.at[place],
            send_sem=lse_send_sem.at[which],
            recv_sem=lse_sem.at[place],
            device_id=(seq, grp),
            device_id_type=MESH,
        )

    @pl.when(gets)
    def _():
        lse_copy(1, 2 * (1 - k), lse_peer).start()

    lse_copy(0, 2 * k, partner).start()

    def w_copy(which, seq):
        rows = pl.ds(pl.multiple_of(k * 128 + which * 64, 64), 64)
        return pltpu.make_async_remote_copy(
            src_ref=w_hbm.at[rows],
            dst_ref=w_other.at[rows],
            send_sem=w_send_sem.at[which],
            recv_sem=w_sem.at[which],
            device_id=(seq, other),
            device_id_type=MESH,
        )

    def w_relay():
        rows = pl.ds(pl.multiple_of(k * 128, 128), 128)
        return pltpu.make_async_remote_copy(
            src_ref=w_other.at[rows],
            dst_ref=w_other.at[rows],
            send_sem=w_send_sem.at[2],
            recv_sem=w_sem.at[2],
            device_id=(partner, grp),
            device_id_type=MESH,
        )

    w_copy(0, me).start()
    w_copy(1, across).start()

    vals.ring_arrived()
    for b in range(4):
        total = None
        for tile in square:
            if tile[1] == b:
                part = numerator_tile(tile)
                total = part if total is None else total + part
        acc[b] = total

    def add_side(right, tile_of):
        work = side(right)
        for q in (3, 2, 1, 0):
            first = q * (q + 1) // 2
            b = work[first][1]
            total = acc[b]
            for tile in work[first : first + q + 1]:
                total = total + tile_of(tile)
            acc[b] = total

    add_side(near, numerator_tile)
    grads.relay()
    vals.halo_arrived()
    add_side(far, numerator_tile)
    for b in range(4):
        att[b] = (acc[b] * (1.0 / tot[b])).astype(jnp.bfloat16)

    def att_copy(b, head):
        return pltpu.make_async_remote_copy(
            src_ref=att.at[b, :, pl.ds(pl.multiple_of(head * 128, 128), 128)],
            dst_ref=att_recv.at[grp * 4 + y],
            send_sem=att_send_sem.at[b, head],
            recv_sem=att_sem.at[grp * 4 + y],
            device_id=(ring * RING + 4 * k + b, head),
            device_id_type=MESH,
        )

    def owner(b):
        return ring * RING + 4 * k + b

    for b in range(4):
        att_copy(b, other).start()

        @pl.when(jnp.logical_not(owner(b) == me))
        def _():
            att_copy(b, grp).start()

    @pl.when(home == k)
    def _():
        b = inner - 4 * k
        att_recv[grp * 4 + y] = att[b, :, pl.ds(pl.multiple_of(grp * 128, 128), 128)]

    def turn_lse(place):
        for row in range(4):
            value = jnp.broadcast_to(lse[place, pl.ds(row, 1), :], (128, TOK))
            columns[4 * place + row] = value.T

    def backward_tile(tile):
        slot, b, place, distance = tile
        column = columns[slot]
        shifted = tiles[place] - jnp.concatenate([column, column], axis=1)
        share = jnp.exp(shifted).astype(jnp.bfloat16)
        part = jnp.dot(buf_g[slot], share, preferred_element_type=jnp.float32)
        if distance is None:
            return part
        return jnp.where(allowed_row(slot, b, distance), part, 0.0)

    grads.ring_arrived()
    turn_lse(1)
    for b in range(4):
        total = None
        for tile in square:
            if tile[1] == b:
                part = backward_tile(tile)
                total = part if total is None else total + part
        acc[b] = total

    lse_copy(0, 2 * near, partner).wait_recv()
    turn_lse(2 * near)
    add_side(near, backward_tile)
    @pl.when(gets)
    def _():
        lse_copy(0, 2 * far, partner).wait_recv()

    grads.halo_arrived()
    turn_lse(2 * far)
    add_side(far, backward_tile)

    for b in range(4):
        vg[b] = acc[b].astype(jnp.bfloat16)

    def vg_copy(b):
        return pltpu.make_async_remote_copy(
            src_ref=vg.at[b],
            dst_ref=vg_recv.at[y],
            send_sem=vg_send_sem.at[b],
            recv_sem=vg_sem.at[y],
            device_id=(owner(b), grp),
            device_id_type=MESH,
        )

    for b in range(4):

        @pl.when(jnp.logical_not(owner(b) == me))
        def _():
            vg_copy(b).start()

    @pl.when(home == k)
    def _():
        vg_recv[y] = vg[inner - 4 * k]

    w_copy(0, me).wait_recv()
    w_copy(1, across).wait_recv()
    w_relay().start()

    def att_arrived(place):
        pltpu.make_async_remote_copy(
            src_ref=att.at[0, :, pl.ds(0, 128)],
            dst_ref=att_recv.at[place],
            send_sem=att_send_sem.at[0, 0],
            recv_sem=att_sem.at[place],
            device_id=(me, other),
            device_id_type=MESH,
        ).wait_recv()

    for h in range(4):
        att_arrived(other * 4 + h)

        @pl.when(jnp.logical_not(ring * RING + 2 * h + home == me))
        def _():
            att_arrived(grp * 4 + h)

    w_relay().wait_recv()
    loads[4].wait()
    mine = att_recv[pl.ds(grp * 4, 4)].reshape(4 * HD, 128).T
    theirs = att_recv[pl.ds(other * 4, 4)].reshape(4 * HD, 128).T
    mixed_ref[...] = (
        jnp.dot(mine, w_ref[...], preferred_element_type=jnp.float32)
        + jnp.dot(theirs, w_other[...], preferred_element_type=jnp.float32)
    ).astype(jnp.bfloat16)

    for h in range(4):

        @pl.when(jnp.logical_not(ring * RING + 2 * h + home == me))
        def _():
            pltpu.make_async_remote_copy(
                src_ref=vg.at[0],
                dst_ref=vg_recv.at[h],
                send_sem=vg_send_sem.at[0],
                recv_sem=vg_sem.at[h],
                device_id=(partner, grp),
                device_id_type=MESH,
            ).wait_recv()

    vgrad_ref[...] = vg_recv[...].reshape(4 * HD, TOK).T

    for stream in (keys, vals, grads):
        stream.finish()
    w_copy(0, me).wait_send()
    w_copy(1, across).wait_send()
    w_relay().wait_send()
    lse_copy(0, 0, partner).wait_send()

    @pl.when(gets)
    def _():
        lse_copy(1, 0, partner).wait_send()

    for b in range(4):
        att_copy(b, other).wait_send()

        @pl.when(jnp.logical_not(owner(b) == me))
        def _():
            att_copy(b, grp).wait_send()
            vg_copy(b).wait_send()


def shards(queries, values, scales, block_reach, out_weight, out_grad):
    vmem = pl.BlockSpec(memory_space=pltpu.VMEM)
    hbm = pl.BlockSpec(memory_space=pltpu.HBM)

    def in_hbm(array):
        return pltpu.with_memory_space_constraint(array, pltpu.HBM)

    bf16, f32 = jnp.bfloat16, jnp.float32
    dma = pltpu.SemaphoreType.DMA
    return pl.pallas_call(
        kernel,
        out_shape=(
            jax.ShapeDtypeStruct((TOK // 2, D), bf16),
            jax.ShapeDtypeStruct((TOK, HEADS_DEV * HD), bf16),
        ),
        in_specs=[hbm, hbm, hbm, hbm, pl.BlockSpec(memory_space=pltpu.SMEM), hbm],
        out_specs=(vmem, vmem),
        scratch_shapes=[
            pltpu.VMEM((TOK, HEADS_DEV * HD), bf16),
            pltpu.VMEM((TOK, HEADS_DEV * HD), bf16),
            pltpu.VMEM((TOK, HEADS_DEV * HD), bf16),
            pltpu.VMEM((HEADS_DEV, TOK), f32),
            pltpu.VMEM((HEADS_DEV * HD, D), bf16),
            pltpu.VMEM((4, ROWS, HALF), bf16),
            pltpu.VMEM((4, HD, TOK), bf16),
            pltpu.VMEM((4, HD, TOK), bf16),
            pltpu.VMEM((12, ROWS, HALF), bf16),
            pltpu.VMEM((12, HD, TOK), bf16),
            pltpu.VMEM((12, HD, TOK), bf16),
            pltpu.VMEM((12, TOK, HD), bf16),
            pltpu.VMEM((36, TOK, TOK), f32),
            pltpu.VMEM((36, TOK, TOK), bf16),
            pltpu.VMEM((12, TOK, 128), f32),
            pltpu.VMEM((36, 1, TOK), f32),
            pltpu.VMEM((4, 1, TOK), f32),
            pltpu.VMEM((4, 1, TOK), f32),
            pltpu.VMEM((4, HD, TOK), f32),
            pltpu.VMEM((3, 8, TOK), f32),
            pltpu.VMEM((4, HD, TOK), bf16),
            pltpu.VMEM((8, HD, TOK // 2), bf16),
            pltpu.VMEM((4, HD, TOK), bf16),
            pltpu.VMEM((4, HD, TOK), bf16),
            pltpu.VMEM((TOK, D), bf16),
            dma((12,)),
            dma((11,)),
            dma((12,)),
            dma((11,)),
            dma((12,)),
            dma((11,)),
            dma((3,)),
            dma((2,)),
            dma((8,)),
            dma((4, 2)),
            dma((4,)),
            dma((4,)),
            dma((3,)),
            dma((3,)),
            dma((5,)),
        ],
        compiler_params=pltpu.CompilerParams(
            collective_id=0, has_side_effects=True, vmem_limit_bytes=40 * 1024 * 1024
        ),
    )(
        in_hbm(queries),
        in_hbm(values),
        in_hbm(out_grad),
        in_hbm(scales.T),
        block_reach,
        in_hbm(out_weight),
    )


def solution(mesh):
    return jax.shard_map(
        shards,
        mesh=mesh,
        in_specs=(
            P("seq", "head"),
            P("seq", "head"),
            P("seq", "head"),
            P("seq"),
            P("head", None),
            P("seq", "head"),
        ),
        out_specs=(P(("seq", "head"), None), P("seq", "head")),
        check_vma=False,
    )
```

```python
import jax
import jax.numpy as jnp
from jax import lax
from jax.experimental import pallas as pl
from jax.experimental.pallas import tpu as pltpu
from jax.sharding import PartitionSpec as P

HD = 64
TOK = 256
HEADS_DEV = 4
D = 1024
RINGS = 16
RING = 8
NBLK = 128
ROWS = 2 * HD + 16
HALF = TOK // 2
MESH = pl.DeviceIdType.MESH
START = -1e30
NEGATIVE = -1e30
BARRED = -3e30


def kernel(
    q_hbm,
    v_hbm,
    g_hbm,
    scale_hbm,
    reach_ref,
    w_hbm,
    mixed_ref,
    vgrad_ref,
    q_ref,
    v_ref,
    g_ref,
    scale_ref,
    w_ref,
    send,
    send_v,
    send_g,
    buf,
    buf_v,
    buf_g,
    kf,
    tiles,
    weights,
    columns,
    tile_tops,
    top,
    tot,
    acc,
    lse,
    att,
    att_recv,
    vg,
    vg_recv,
    w_other,
    slot_sem,
    send_sem,
    slot_v_sem,
    send_v_sem,
    slot_g_sem,
    send_g_sem,
    lse_sem,
    lse_send_sem,
    att_sem,
    att_send_sem,
    vg_sem,
    vg_send_sem,
    w_sem,
    w_send_sem,
    in_sem,
):
    me = lax.axis_index("seq")
    grp = lax.axis_index("head")
    ring = me // RING
    inner = me % RING
    y = inner // 2
    k = inner % 2
    other = 1 - grp
    home = y // 2
    partner = me + 1 - 2 * k
    prev_ring = ((ring + RINGS - 1) % RINGS) * RING
    next_ring = ((ring + 1) % RINGS) * RING
    up = y // 2
    across = me + RING - 2 * RING * (ring % 2)

    halo_from = prev_ring * (1 - k) + next_ring * k + 4 * (1 - k)
    lse_peer = (prev_ring + 2 * y + 1) * (1 - k) + (next_ring + 2 * y) * k
    halo_to = (next_ring) * up + (prev_ring + 1) * (1 - up)
    halo_slot = (2 * y + k - 4) * up + (2 * y + k + 8) * (1 - up)
    own_slot = 2 * y + 4 - 3 * k
    partner_slot = 2 * y + 5 * k
    is_home = (home == k).astype(jnp.int32)
    first, last = ring == 0, ring == RINGS - 1
    gets = jnp.logical_not(jnp.logical_or(jnp.logical_and(first, k == 0), jnp.logical_and(last, k == 1)))
    gives = jnp.logical_not(jnp.logical_or(jnp.logical_and(first, up == 0), jnp.logical_and(last, up == 1)))
    expected = 14 - is_home + gets.astype(jnp.int32) + 4 * gives.astype(jnp.int32)

    barrier = pltpu.get_barrier_semaphore()
    loads = [
        pltpu.make_async_copy(source, target, in_sem.at[i])
        for i, (source, target) in enumerate(
            (
                (q_hbm, q_ref),
                (scale_hbm, scale_ref),
                (v_hbm, v_ref),
                (g_hbm, g_ref),
                (w_hbm, w_ref),
            )
        )
    ]
    for load in loads:
        load.start()

    def greet(seq, head):
        pl.semaphore_signal(barrier, inc=1, device_id=(seq, head), device_id_type=MESH)

    greet(partner, grp)
    for step in range(1, 4):
        greet(ring * RING + 2 * ((y + step) % 4) + k, grp)

    @pl.when(gets)
    def _():
        for j in range(4):
            greet(halo_from + j, grp)
        greet(lse_peer, grp)

    for h in range(4):
        source = ring * RING + 2 * h + home
        greet(source, other)

        @pl.when(jnp.logical_not(source == me))
        def _():
            greet(source, grp)

    greet(me, other)
    greet(across, other)

    for load in loads[:4]:
        load.wait()
    q_t = q_ref[...].T
    v_t = v_ref[...].T
    g_t = g_ref[...].T
    reach_rows = jnp.full((16, HALF), reach_ref[0].astype(jnp.float32)).astype(jnp.bfloat16)
    for h in range(HEADS_DEV):
        part = q_t[h * HD : (h + 1) * HD, :].astype(jnp.float32)
        square = jnp.sum(part * part, axis=0, keepdims=True)
        direction = part * lax.rsqrt(square + 1e-06)
        key = (direction * scale_ref[h : h + 1, :]).astype(jnp.bfloat16)
        send[h, 0:HD, :] = key[:, 0:HALF]
        send[h, HD : 2 * HD, :] = key[:, HALF:]
        send[h, 2 * HD :, :] = reach_rows
        send_v[h] = v_t[h * HD : (h + 1) * HD, :]
        send_g[h] = g_t[h * HD : (h + 1) * HD, :]

    pl.semaphore_wait(barrier, expected)

    class Stream:
        def __init__(self, source, place, arrive, sent):
            self.source, self.place, self.arrive, self.sent = source, place, arrive, sent

        def copy(self, src, slot, which, seq):
            return pltpu.make_async_remote_copy(
                src_ref=src,
                dst_ref=self.place.at[slot],
                send_sem=self.sent.at[which],
                recv_sem=self.arrive.at[slot],
                device_id=(seq, grp),
                device_id_type=MESH,
            )

        def start(self):
            for step in (2, 1, 3):
                target = (y + step) % 4
                self.copy(
                    self.source.at[target], own_slot, step, ring * RING + 2 * target + k
                ).start()
            self.copy(self.source.at[y], partner_slot, 0, partner).start()

            @pl.when(gives)
            def _():
                for step in (0, 1, 3, 2):
                    target = (y + step) % 4
                    self.copy(
                        self.source.at[target], halo_slot, 4 + step, halo_to + 2 * target
                    ).start()

        def arrived(self, slot):
            self.copy(self.source.at[0], slot, 0, partner).wait_recv()

        def relay(self):
            for step in (1, 3, 2):
                source = (y + step) % 4
                slot = 2 * source + 4 - 3 * k
                self.arrived(slot)
                self.copy(self.place.at[slot], 2 * source + 5 * k, 7 + step, partner).start()

        def ring_arrived(self):
            for source in range(4):
                self.arrived(2 * source + 5 - 5 * k)

        def halo_arrived(self):
            @pl.when(gets)
            def _():
                for m in range(4):
                    self.arrived((8 + m) * k + (3 - m) * (1 - k))

        def finish(self):
            for which in (0, 1, 2, 3, 8, 9, 10):
                self.copy(self.source.at[0], 0, which, partner).wait_send()

            @pl.when(gives)
            def _():
                for which in range(4, 8):
                    self.copy(self.source.at[0], 0, which, partner).wait_send()

    keys = Stream(send, buf, slot_sem, send_sem)
    vals = Stream(send_v, buf_v, slot_v_sem, send_v_sem)
    grads = Stream(send_g, buf_g, slot_g_sem, send_g_sem)
    for stream in (keys, vals, grads):
        stream.start()
    buf[own_slot] = send[y]
    buf_v[own_slot] = send_v[y]
    buf_g[own_slot] = send_g[y]

    @pl.when(jnp.logical_not(gets))
    def _():
        for m in range(4):
            slot = (8 + m) * k + m * (1 - k)
            buf[slot] = jnp.zeros((ROWS, HALF), jnp.bfloat16)
            buf_v[slot] = jnp.zeros((HD, TOK), jnp.bfloat16)
            buf_g[slot] = jnp.zeros((HD, TOK), jnp.bfloat16)
        lse[2 * k] = jnp.zeros((8, TOK), jnp.float32)

    keys.relay()
    keys.ring_arrived()

    def key_of(slot):
        return jnp.concatenate([buf[slot, 0:HD, :], buf[slot, HD : 2 * HD, :]], axis=1)

    def turn(slot):
        kf[slot] = key_of(slot).T

    first_block = ring * RING + 4 * k - 4

    def allowed_row(slot, b, distance):
        index = first_block + slot
        valid = jnp.logical_and(index >= 0, index < NBLK)
        needed = jnp.where(valid, distance, 99).astype(jnp.float32)
        far = buf[slot, 2 * HD :, :].astype(jnp.float32)[0:1]
        mine = buf[4 + b, 2 * HD :, :].astype(jnp.float32)[0:1]
        row = needed <= jnp.minimum(far, mine)
        return jnp.concatenate([row, row], axis=1)

    def score_tile(tile):
        slot, b, place, distance = tile
        scores = jnp.dot(kf[slot], key_of(4 + b), preferred_element_type=jnp.float32)
        if distance is None:
            row = lax.broadcasted_iota(jnp.int32, (TOK, TOK), 0)
            column = lax.broadcasted_iota(jnp.int32, (TOK, TOK), 1)
            scores = jnp.where(row == column, NEGATIVE, scores)
        tiles[place] = scores

    def exponent_tile(tile):
        slot, b, place, distance = tile
        scores = tiles[place]
        tile_top = jnp.max(scores, axis=0, keepdims=True)
        exponent = jnp.exp(scores - tile_top)
        weights[place] = exponent.astype(jnp.bfloat16)
        tile_sum = jnp.sum(exponent, axis=0, keepdims=True)
        if distance is None:
            tile_tops[place], top[b], tot[b] = tile_top, tile_top, tile_sum
            return
        tile_top = jnp.where(allowed_row(slot, b, distance), tile_top, BARRED)
        new_top = jnp.maximum(top[b], tile_top)
        tile_tops[place] = tile_top
        tot[b] = jnp.exp(top[b] - new_top) * tot[b] + jnp.exp(tile_top - new_top) * tile_sum
        top[b] = new_top

    def exponents(work):
        for t in range(len(work) + 2):
            if t >= 2:
                exponent_tile(work[t - 2])
            if t < len(work):
                score_tile(work[t])

    def numerator_tile(tile):
        slot, b, place, _ = tile
        part = jnp.dot(buf_v[slot], weights[place], preferred_element_type=jnp.float32)
        return jnp.exp(tile_tops[place] - top[b]) * part

    square = [
        (4 + i, (i + step) % 4, 9 * ((i + step) % 4) + 4 + i - (i + step) % 4, abs(i - (i + step) % 4) or None)
        for step in range(4)
        for i in range(4)
    ]

    def side(right):
        work = []
        for q in range(4):
            for m in range(q + 1):
                slot = (8 + m) * right + (3 - m) * (1 - right)
                b = q * right + (3 - q) * (1 - right)
                work.append((slot, b, 9 * b + slot - b, 4 + m - q))
        return work

    near, far = 1 - k, k

    for i in range(8):
        turn(i + 4 * near)
    exponents(square + side(near))
    vals.relay()
    loads[4].wait()
    def w_copy(which, seq):
        rows = pl.ds(pl.multiple_of(k * 128 + which * 64, 64), 64)
        return pltpu.make_async_remote_copy(
            src_ref=w_ref.at[rows],
            dst_ref=w_other.at[rows],
            send_sem=w_send_sem.at[which],
            recv_sem=w_sem.at[which],
            device_id=(seq, other),
            device_id_type=MESH,
        )

    def w_relay():
        rows = pl.ds(pl.multiple_of(k * 128, 128), 128)
        return pltpu.make_async_remote_copy(
            src_ref=w_other.at[rows],
            dst_ref=w_other.at[rows],
            send_sem=w_send_sem.at[2],
            recv_sem=w_sem.at[2],
            device_id=(partner, grp),
            device_id_type=MESH,
        )

    w_copy(0, me).start()
    w_copy(1, across).start()

    keys.halo_arrived()
    for m in range(4):
        turn((8 + m) * far + (3 - m) * (1 - far))
    exponents(side(far))

    denominators = [top[b] + jnp.log(tot[b]) for b in range(4)]
    lse[1] = jnp.concatenate(denominators + denominators, axis=0)

    def lse_copy(which, place, seq):
        return pltpu.make_async_remote_copy(
            src_ref=lse.at[1],
            dst_ref=lse.at[place],
            send_sem=lse_send_sem.at[which],
            recv_sem=lse_sem.at[place],
            device_id=(seq, grp),
            device_id_type=MESH,
        )

    @pl.when(gets)
    def _():
        lse_copy(1, 2 * (1 - k), lse_peer).start()

    lse_copy(0, 2 * k, partner).start()

    grads.relay()
    vals.ring_arrived()
    for b in range(4):
        total = None
        for tile in square:
            if tile[1] == b:
                part = numerator_tile(tile)
                total = part if total is None else total + part
        acc[b] = total

    def add_side(right, tile_of):
        work = side(right)
        for q in (3, 2, 1, 0):
            first = q * (q + 1) // 2
            b = work[first][1]
            total = acc[b]
            for tile in work[first : first + q + 1]:
                total = total + tile_of(tile)
            acc[b] = total

    add_side(near, numerator_tile)
    vals.halo_arrived()
    add_side(far, numerator_tile)
    for b in range(4):
        att[b] = (acc[b] * (1.0 / tot[b])).astype(jnp.bfloat16)

    def att_copy(b, head):
        return pltpu.make_async_remote_copy(
            src_ref=att.at[b, :, pl.ds(pl.multiple_of(head * 128, 128), 128)],
            dst_ref=att_recv.at[grp * 4 + y],
            send_sem=att_send_sem.at[b, head],
            recv_sem=att_sem.at[grp * 4 + y],
            device_id=(ring * RING + 4 * k + b, head),
            device_id_type=MESH,
        )

    def owner(b):
        return ring * RING + 4 * k + b

    for b in range(4):
        att_copy(b, other).start()

        @pl.when(jnp.logical_not(owner(b) == me))
        def _():
            att_copy(b, grp).start()

    @pl.when(home == k)
    def _():
        b = inner - 4 * k
        att_recv[grp * 4 + y] = att[b, :, pl.ds(pl.multiple_of(grp * 128, 128), 128)]

    def turn_lse(place):
        for row in range(4):
            value = jnp.broadcast_to(lse[place, pl.ds(row, 1), :], (128, TOK))
            columns[4 * place + row] = value.T

    def backward_tile(tile):
        slot, b, place, distance = tile
        column = columns[slot]
        shifted = tiles[place] - jnp.concatenate([column, column], axis=1)
        share = jnp.exp(shifted).astype(jnp.bfloat16)
        part = jnp.dot(buf_g[slot], share, preferred_element_type=jnp.float32)
        if distance is None:
            return part
        return jnp.where(allowed_row(slot, b, distance), part, 0.0)

    grads.ring_arrived()
    turn_lse(1)
    for b in range(4):
        total = None
        for tile in square:
            if tile[1] == b:
                part = backward_tile(tile)
                total = part if total is None else total + part
        acc[b] = total

    lse_copy(0, 2 * near, partner).wait_recv()
    turn_lse(2 * near)
    add_side(near, backward_tile)
    @pl.when(gets)
    def _():
        lse_copy(0, 2 * far, partner).wait_recv()

    grads.halo_arrived()
    turn_lse(2 * far)
    add_side(far, backward_tile)

    for b in range(4):
        vg[b] = acc[b].astype(jnp.bfloat16)

    def vg_copy(b):
        return pltpu.make_async_remote_copy(
            src_ref=vg.at[b],
            dst_ref=vg_recv.at[y],
            send_sem=vg_send_sem.at[b],
            recv_sem=vg_sem.at[y],
            device_id=(owner(b), grp),
            device_id_type=MESH,
        )

    for b in range(4):

        @pl.when(jnp.logical_not(owner(b) == me))
        def _():
            vg_copy(b).start()

    @pl.when(home == k)
    def _():
        vg_recv[y] = vg[inner - 4 * k]

    w_copy(0, me).wait_recv()
    w_copy(1, across).wait_recv()
    w_relay().start()

    def att_arrived(place):
        pltpu.make_async_remote_copy(
            src_ref=att.at[0, :, pl.ds(0, 128)],
            dst_ref=att_recv.at[place],
            send_sem=att_send_sem.at[0, 0],
            recv_sem=att_sem.at[place],
            device_id=(me, other),
            device_id_type=MESH,
        ).wait_recv()

    for h in range(4):
        att_arrived(other * 4 + h)

        @pl.when(jnp.logical_not(ring * RING + 2 * h + home == me))
        def _():
            att_arrived(grp * 4 + h)

    w_relay().wait_recv()
    mine = att_recv[pl.ds(grp * 4, 4)].reshape(4 * HD, 128).T
    theirs = att_recv[pl.ds(other * 4, 4)].reshape(4 * HD, 128).T
    mixed_ref[...] = (
        jnp.dot(mine, w_ref[...], preferred_element_type=jnp.float32)
        + jnp.dot(theirs, w_other[...], preferred_element_type=jnp.float32)
    ).astype(jnp.bfloat16)

    for h in range(4):

        @pl.when(jnp.logical_not(ring * RING + 2 * h + home == me))
        def _():
            pltpu.make_async_remote_copy(
                src_ref=vg.at[0],
                dst_ref=vg_recv.at[h],
                send_sem=vg_send_sem.at[0],
                recv_sem=vg_sem.at[h],
                device_id=(partner, grp),
                device_id_type=MESH,
            ).wait_recv()

    vgrad_ref[...] = vg_recv[...].reshape(4 * HD, TOK).T

    for stream in (keys, vals, grads):
        stream.finish()
    w_copy(0, me).wait_send()
    w_copy(1, across).wait_send()
    w_relay().wait_send()
    lse_copy(0, 0, partner).wait_send()

    @pl.when(gets)
    def _():
        lse_copy(1, 0, partner).wait_send()

    for b in range(4):
        att_copy(b, other).wait_send()

        @pl.when(jnp.logical_not(owner(b) == me))
        def _():
            att_copy(b, grp).wait_send()
            vg_copy(b).wait_send()


def store(mixed_vmem, vgrad_vmem, mixed_hbm, vgrad_hbm, sem):
    copies = [
        pltpu.make_async_copy(mixed_vmem, mixed_hbm, sem.at[0]),
        pltpu.make_async_copy(vgrad_vmem, vgrad_hbm, sem.at[1]),
    ]
    for copy in copies:
        copy.start()
    for copy in copies:
        copy.wait()


def shards(queries, values, scales, block_reach, out_weight, out_grad):
    vmem = pl.BlockSpec(memory_space=pltpu.VMEM)
    hbm = pl.BlockSpec(memory_space=pltpu.HBM)

    def in_hbm(array):
        return pltpu.with_memory_space_constraint(array, pltpu.HBM)

    bf16, f32 = jnp.bfloat16, jnp.float32
    dma = pltpu.SemaphoreType.DMA
    mixed, vgrad = pl.pallas_call(
        kernel,
        out_shape=(
            jax.ShapeDtypeStruct((TOK // 2, D), bf16),
            jax.ShapeDtypeStruct((TOK, HEADS_DEV * HD), bf16),
        ),
        in_specs=[hbm, hbm, hbm, hbm, pl.BlockSpec(memory_space=pltpu.SMEM), hbm],
        out_specs=(vmem, vmem),
        scratch_shapes=[
            pltpu.VMEM((TOK, HEADS_DEV * HD), bf16),
            pltpu.VMEM((TOK, HEADS_DEV * HD), bf16),
            pltpu.VMEM((TOK, HEADS_DEV * HD), bf16),
            pltpu.VMEM((HEADS_DEV, TOK), f32),
            pltpu.VMEM((HEADS_DEV * HD, D), bf16),
            pltpu.VMEM((4, ROWS, HALF), bf16),
            pltpu.VMEM((4, HD, TOK), bf16),
            pltpu.VMEM((4, HD, TOK), bf16),
            pltpu.VMEM((12, ROWS, HALF), bf16),
            pltpu.VMEM((12, HD, TOK), bf16),
            pltpu.VMEM((12, HD, TOK), bf16),
            pltpu.VMEM((12, TOK, HD), bf16),
            pltpu.VMEM((36, TOK, TOK), f32),
            pltpu.VMEM((36, TOK, TOK), bf16),
            pltpu.VMEM((12, TOK, 128), f32),
            pltpu.VMEM((36, 1, TOK), f32),
            pltpu.VMEM((4, 1, TOK), f32),
            pltpu.VMEM((4, 1, TOK), f32),
            pltpu.VMEM((4, HD, TOK), f32),
            pltpu.VMEM((3, 8, TOK), f32),
            pltpu.VMEM((4, HD, TOK), bf16),
            pltpu.VMEM((8, HD, TOK // 2), bf16),
            pltpu.VMEM((4, HD, TOK), bf16),
            pltpu.VMEM((4, HD, TOK), bf16),
            pltpu.VMEM((TOK, D), bf16),
            dma((12,)),
            dma((11,)),
            dma((12,)),
            dma((11,)),
            dma((12,)),
            dma((11,)),
            dma((3,)),
            dma((2,)),
            dma((8,)),
            dma((4, 2)),
            dma((4,)),
            dma((4,)),
            dma((3,)),
            dma((3,)),
            dma((5,)),
        ],
        compiler_params=pltpu.CompilerParams(
            collective_id=0, has_side_effects=True, vmem_limit_bytes=40 * 1024 * 1024
        ),
    )(
        in_hbm(queries),
        in_hbm(values),
        in_hbm(out_grad),
        in_hbm(scales.T),
        block_reach,
        in_hbm(out_weight),
    )
    return pl.pallas_call(
        store,
        out_shape=(
            jax.ShapeDtypeStruct((TOK // 2, D), bf16),
            jax.ShapeDtypeStruct((TOK, HEADS_DEV * HD), bf16),
        ),
        in_specs=[vmem, vmem],
        out_specs=(hbm, hbm),
        scratch_shapes=[dma((2,))],
    )(
        pltpu.with_memory_space_constraint(mixed, pltpu.VMEM),
        pltpu.with_memory_space_constraint(vgrad, pltpu.VMEM),
    )


def solution(mesh):
    return jax.shard_map(
        shards,
        mesh=mesh,
        in_specs=(
            P("seq", "head"),
            P("seq", "head"),
            P("seq", "head"),
            P("seq"),
            P("head", None),
            P("seq", "head"),
        ),
        out_specs=(P(("seq", "head"), None), P("seq", "head")),
        check_vma=False,
    )
```

```python
import jax
import jax.numpy as jnp
from jax import lax
from jax.experimental import pallas as pl
from jax.experimental.pallas import tpu as pltpu
from jax.sharding import PartitionSpec as P

HD = 64
TOK = 256
HEADS_DEV = 4
D = 1024
RINGS = 16
RING = 8
NBLK = 128
ROWS = 2 * HD + 16
HALF = TOK // 2
MESH = pl.DeviceIdType.MESH
START = -1e30
NEGATIVE = -1e30
BARRED = -3e30


def kernel(
    q_hbm,
    v_hbm,
    g_hbm,
    scale_hbm,
    reach_ref,
    w_hbm,
    mixed_ref,
    vgrad_ref,
    q_ref,
    v_ref,
    g_ref,
    scale_ref,
    w_ref,
    send,
    send_v,
    send_g,
    buf,
    buf_v,
    buf_g,
    kf,
    tiles,
    weights,
    columns,
    tile_tops,
    top,
    tot,
    acc,
    lse,
    att,
    att_recv,
    vg,
    vg_recv,
    w_other,
    slot_sem,
    send_sem,
    slot_v_sem,
    send_v_sem,
    slot_g_sem,
    send_g_sem,
    lse_sem,
    lse_send_sem,
    att_sem,
    att_send_sem,
    vg_sem,
    vg_send_sem,
    w_sem,
    w_send_sem,
    in_sem,
):
    me = lax.axis_index("seq")
    grp = lax.axis_index("head")
    ring = me // RING
    inner = me % RING
    y = inner // 2
    k = inner % 2
    other = 1 - grp
    home = y // 2
    partner = me + 1 - 2 * k
    prev_ring = ((ring + RINGS - 1) % RINGS) * RING
    next_ring = ((ring + 1) % RINGS) * RING
    up = y // 2
    across = me + RING - 2 * RING * (ring % 2)

    halo_from = prev_ring * (1 - k) + next_ring * k + 4 * (1 - k)
    lse_peer = (prev_ring + 2 * y + 1) * (1 - k) + (next_ring + 2 * y) * k
    halo_to = (next_ring) * up + (prev_ring + 1) * (1 - up)
    halo_slot = (2 * y + k - 4) * up + (2 * y + k + 8) * (1 - up)
    own_slot = 2 * y + 4 - 3 * k
    partner_slot = 2 * y + 5 * k
    is_home = (home == k).astype(jnp.int32)
    first, last = ring == 0, ring == RINGS - 1
    gets = jnp.logical_not(jnp.logical_or(jnp.logical_and(first, k == 0), jnp.logical_and(last, k == 1)))
    gives = jnp.logical_not(jnp.logical_or(jnp.logical_and(first, up == 0), jnp.logical_and(last, up == 1)))
    expected = 14 - is_home + gets.astype(jnp.int32) + 4 * gives.astype(jnp.int32)

    barrier = pltpu.get_barrier_semaphore()
    loads = [
        pltpu.make_async_copy(source, target, in_sem.at[i])
        for i, (source, target) in enumerate(
            (
                (q_hbm, q_ref),
                (scale_hbm, scale_ref),
                (v_hbm, v_ref),
                (g_hbm, g_ref),
                (w_hbm, w_ref),
            )
        )
    ]
    for load in loads:
        load.start()

    def greet(seq, head):
        pl.semaphore_signal(barrier, inc=1, device_id=(seq, head), device_id_type=MESH)

    greet(partner, grp)
    for step in range(1, 4):
        greet(ring * RING + 2 * ((y + step) % 4) + k, grp)

    @pl.when(gets)
    def _():
        for j in range(4):
            greet(halo_from + j, grp)
        greet(lse_peer, grp)

    for h in range(4):
        source = ring * RING + 2 * h + home
        greet(source, other)

        @pl.when(jnp.logical_not(source == me))
        def _():
            greet(source, grp)

    greet(me, other)
    greet(across, other)

    for load in loads[:4]:
        load.wait()
    q_t = q_ref[...].T
    v_t = v_ref[...].T
    g_t = g_ref[...].T
    reach_rows = jnp.full((16, HALF), reach_ref[0].astype(jnp.float32)).astype(jnp.bfloat16)
    for h in range(HEADS_DEV):
        part = q_t[h * HD : (h + 1) * HD, :].astype(jnp.float32)
        square = jnp.sum(part * part, axis=0, keepdims=True)
        direction = part * lax.rsqrt(square + 1e-06)
        key = (direction * scale_ref[h : h + 1, :]).astype(jnp.bfloat16)
        send[h, 0:HD, :] = key[:, 0:HALF]
        send[h, HD : 2 * HD, :] = key[:, HALF:]
        send[h, 2 * HD :, :] = reach_rows
        send_v[h] = v_t[h * HD : (h + 1) * HD, :]
        send_g[h] = g_t[h * HD : (h + 1) * HD, :]

    pl.semaphore_wait(barrier, expected)

    class Stream:
        def __init__(self, source, place, arrive, sent):
            self.source, self.place, self.arrive, self.sent = source, place, arrive, sent

        def copy(self, src, slot, which, seq):
            return pltpu.make_async_remote_copy(
                src_ref=src,
                dst_ref=self.place.at[slot],
                send_sem=self.sent.at[which],
                recv_sem=self.arrive.at[slot],
                device_id=(seq, grp),
                device_id_type=MESH,
            )

        def start(self):
            for step in (2, 1, 3):
                target = (y + step) % 4
                self.copy(
                    self.source.at[target], own_slot, step, ring * RING + 2 * target + k
                ).start()
            self.copy(self.source.at[y], partner_slot, 0, partner).start()

            @pl.when(gives)
            def _():
                for step in (0, 1, 3, 2):
                    target = (y + step) % 4
                    self.copy(
                        self.source.at[target], halo_slot, 4 + step, halo_to + 2 * target
                    ).start()

        def arrived(self, slot):
            self.copy(self.source.at[0], slot, 0, partner).wait_recv()

        def relay(self, use=None):
            for step in (1, 3, 2):
                source = (y + step) % 4
                slot = 2 * source + 4 - 3 * k
                self.arrived(slot)
                self.copy(self.place.at[slot], 2 * source + 5 * k, 7 + step, partner).start()
                if use is not None:
                    use(slot)

        def ring_arrived(self, use=None):
            for step in (0, 1, 3, 2):
                slot = 2 * ((y + step) % 4) + 5 - 5 * k
                self.arrived(slot)
                if use is not None:
                    use(slot)

        def halo_arrived(self):
            @pl.when(gets)
            def _():
                for m in range(4):
                    self.arrived((8 + m) * k + (3 - m) * (1 - k))

        def finish(self):
            for which in (0, 1, 2, 3, 8, 9, 10):
                self.copy(self.source.at[0], 0, which, partner).wait_send()

            @pl.when(gives)
            def _():
                for which in range(4, 8):
                    self.copy(self.source.at[0], 0, which, partner).wait_send()

    keys = Stream(send, buf, slot_sem, send_sem)
    vals = Stream(send_v, buf_v, slot_v_sem, send_v_sem)
    grads = Stream(send_g, buf_g, slot_g_sem, send_g_sem)
    for stream in (keys, vals, grads):
        stream.start()
    buf[own_slot] = send[y]
    buf_v[own_slot] = send_v[y]
    buf_g[own_slot] = send_g[y]

    @pl.when(jnp.logical_not(gets))
    def _():
        for m in range(4):
            slot = (8 + m) * k + m * (1 - k)
            buf[slot] = jnp.zeros((ROWS, HALF), jnp.bfloat16)
            buf_v[slot] = jnp.zeros((HD, TOK), jnp.bfloat16)
            buf_g[slot] = jnp.zeros((HD, TOK), jnp.bfloat16)
        lse[2 * k] = jnp.zeros((8, TOK), jnp.float32)

    def key_of(slot):
        return jnp.concatenate([buf[slot, 0:HD, :], buf[slot, HD : 2 * HD, :]], axis=1)

    def turn(slot):
        kf[slot] = key_of(slot).T

    turn(own_slot)
    keys.relay(turn)
    keys.ring_arrived(turn)

    first_block = ring * RING + 4 * k - 4

    def allowed_row(slot, b, distance):
        index = first_block + slot
        valid = jnp.logical_and(index >= 0, index < NBLK)
        needed = jnp.where(valid, distance, 99).astype(jnp.float32)
        far = buf[slot, 2 * HD :, :].astype(jnp.float32)[0:1]
        mine = buf[4 + b, 2 * HD :, :].astype(jnp.float32)[0:1]
        row = needed <= jnp.minimum(far, mine)
        return jnp.concatenate([row, row], axis=1)

    def score_tile(tile):
        slot, b, place, distance = tile
        scores = jnp.dot(kf[slot], key_of(4 + b), preferred_element_type=jnp.float32)
        if distance is None:
            row = lax.broadcasted_iota(jnp.int32, (TOK, TOK), 0)
            column = lax.broadcasted_iota(jnp.int32, (TOK, TOK), 1)
            scores = jnp.where(row == column, NEGATIVE, scores)
        tiles[place] = scores

    def exponent_tile(tile):
        slot, b, place, distance = tile
        scores = tiles[place]
        tile_top = jnp.max(scores, axis=0, keepdims=True)
        exponent = jnp.exp(scores - tile_top)
        weights[place] = exponent.astype(jnp.bfloat16)
        tile_sum = jnp.sum(exponent, axis=0, keepdims=True)
        if distance is None:
            tile_tops[place], top[b], tot[b] = tile_top, tile_top, tile_sum
            return
        tile_top = jnp.where(allowed_row(slot, b, distance), tile_top, BARRED)
        new_top = jnp.maximum(top[b], tile_top)
        tile_tops[place] = tile_top
        tot[b] = jnp.exp(top[b] - new_top) * tot[b] + jnp.exp(tile_top - new_top) * tile_sum
        top[b] = new_top

    def exponents(work):
        for t in range(len(work) + 2):
            if t >= 2:
                exponent_tile(work[t - 2])
            if t < len(work):
                score_tile(work[t])

    def numerator_tile(tile):
        slot, b, place, _ = tile
        part = jnp.dot(buf_v[slot], weights[place], preferred_element_type=jnp.float32)
        return jnp.exp(tile_tops[place] - top[b]) * part

    square = [
        (4 + i, (i + step) % 4, 9 * ((i + step) % 4) + 4 + i - (i + step) % 4, abs(i - (i + step) % 4) or None)
        for step in range(4)
        for i in range(4)
    ]

    def side(right):
        work = []
        for q in range(4):
            for m in range(q + 1):
                slot = (8 + m) * right + (3 - m) * (1 - right)
                b = q * right + (3 - q) * (1 - right)
                work.append((slot, b, 9 * b + slot - b, 4 + m - q))
        return work

    near, far = 1 - k, k

    exponents(square + side(near))
    vals.relay()
    loads[4].wait()
    def w_copy(batch, which, seq):
        rows = pl.ds(pl.multiple_of(k * 128 + batch * 64 + which * 32, 32), 32)
        return pltpu.make_async_remote_copy(
            src_ref=w_ref.at[rows],
            dst_ref=w_other.at[rows],
            send_sem=w_send_sem.at[2 * batch + which],
            recv_sem=w_sem.at[2 * batch + which],
            device_id=(seq, other),
            device_id_type=MESH,
        )

    def w_relay(batch):
        rows = pl.ds(pl.multiple_of(k * 128 + batch * 64, 64), 64)
        return pltpu.make_async_remote_copy(
            src_ref=w_other.at[rows],
            dst_ref=w_other.at[rows],
            send_sem=w_send_sem.at[4 + batch],
            recv_sem=w_sem.at[4 + batch],
            device_id=(partner, grp),
            device_id_type=MESH,
        )

    def send_w(batch):
        w_copy(batch, 0, me).start()
        w_copy(batch, 1, across).start()

    def pass_w(batch):
        w_copy(batch, 0, me).wait_recv()
        w_copy(batch, 1, across).wait_recv()
        w_relay(batch).start()

    send_w(0)
    keys.halo_arrived()
    for m in range(4):
        turn((8 + m) * far + (3 - m) * (1 - far))
    exponents(side(far))

    denominators = [top[b] + jnp.log(tot[b]) for b in range(4)]
    lse[1] = jnp.concatenate(denominators + denominators, axis=0)

    def lse_copy(which, place, seq):
        return pltpu.make_async_remote_copy(
            src_ref=lse.at[1],
            dst_ref=lse.at[place],
            send_sem=lse_send_sem.at[which],
            recv_sem=lse_sem.at[place],
            device_id=(seq, grp),
            device_id_type=MESH,
        )

    @pl.when(gets)
    def _():
        lse_copy(1, 2 * (1 - k), lse_peer).start()

    lse_copy(0, 2 * k, partner).start()
    send_w(1)

    grads.relay()
    vals.ring_arrived()
    for b in range(4):
        total = None
        for tile in square:
            if tile[1] == b:
                part = numerator_tile(tile)
                total = part if total is None else total + part
        acc[b] = total

    def add_side(right, tile_of):
        work = side(right)
        for q in (3, 2, 1, 0):
            first = q * (q + 1) // 2
            b = work[first][1]
            total = acc[b]
            for tile in work[first : first + q + 1]:
                total = total + tile_of(tile)
            acc[b] = total

    add_side(near, numerator_tile)
    vals.halo_arrived()
    add_side(far, numerator_tile)
    for b in range(4):
        att[b] = (acc[b] * (1.0 / tot[b])).astype(jnp.bfloat16)

    def att_copy(b, head):
        return pltpu.make_async_remote_copy(
            src_ref=att.at[b, :, pl.ds(pl.multiple_of(head * 128, 128), 128)],
            dst_ref=att_recv.at[grp * 4 + y],
            send_sem=att_send_sem.at[b, head],
            recv_sem=att_sem.at[grp * 4 + y],
            device_id=(ring * RING + 4 * k + b, head),
            device_id_type=MESH,
        )

    def owner(b):
        return ring * RING + 4 * k + b

    for b in range(4):
        att_copy(b, other).start()

        @pl.when(jnp.logical_not(owner(b) == me))
        def _():
            att_copy(b, grp).start()

    @pl.when(home == k)
    def _():
        b = inner - 4 * k
        att_recv[grp * 4 + y] = att[b, :, pl.ds(pl.multiple_of(grp * 128, 128), 128)]

    def turn_lse(place):
        for row in range(4):
            value = jnp.broadcast_to(lse[place, pl.ds(row, 1), :], (128, TOK))
            columns[4 * place + row] = value.T

    def backward_tile(tile):
        slot, b, place, distance = tile
        column = columns[slot]
        shifted = tiles[place] - jnp.concatenate([column, column], axis=1)
        share = jnp.exp(shifted).astype(jnp.bfloat16)
        part = jnp.dot(buf_g[slot], share, preferred_element_type=jnp.float32)
        if distance is None:
            return part
        return jnp.where(allowed_row(slot, b, distance), part, 0.0)

    grads.ring_arrived()
    turn_lse(1)
    for b in range(4):
        total = None
        for tile in square:
            if tile[1] == b:
                part = backward_tile(tile)
                total = part if total is None else total + part
        acc[b] = total

    lse_copy(0, 2 * near, partner).wait_recv()
    turn_lse(2 * near)
    add_side(near, backward_tile)
    @pl.when(gets)
    def _():
        lse_copy(0, 2 * far, partner).wait_recv()

    grads.halo_arrived()
    turn_lse(2 * far)
    add_side(far, backward_tile)

    for b in range(4):
        vg[b] = acc[b].astype(jnp.bfloat16)

    def vg_copy(b):
        return pltpu.make_async_remote_copy(
            src_ref=vg.at[b],
            dst_ref=vg_recv.at[y],
            send_sem=vg_send_sem.at[b],
            recv_sem=vg_sem.at[y],
            device_id=(owner(b), grp),
            device_id_type=MESH,
        )

    for b in range(4):

        @pl.when(jnp.logical_not(owner(b) == me))
        def _():
            vg_copy(b).start()

    @pl.when(home == k)
    def _():
        vg_recv[y] = vg[inner - 4 * k]

    pass_w(0)
    pass_w(1)

    def att_arrived(place):
        pltpu.make_async_remote_copy(
            src_ref=att.at[0, :, pl.ds(0, 128)],
            dst_ref=att_recv.at[place],
            send_sem=att_send_sem.at[0, 0],
            recv_sem=att_sem.at[place],
            device_id=(me, other),
            device_id_type=MESH,
        ).wait_recv()

    for h in range(4):
        att_arrived(other * 4 + h)

        @pl.when(jnp.logical_not(ring * RING + 2 * h + home == me))
        def _():
            att_arrived(grp * 4 + h)

    w_relay(0).wait_recv()
    w_relay(1).wait_recv()
    mine = att_recv[pl.ds(grp * 4, 4)].reshape(4 * HD, 128).T
    theirs = att_recv[pl.ds(other * 4, 4)].reshape(4 * HD, 128).T
    mixed_ref[...] = (
        jnp.dot(mine, w_ref[...], preferred_element_type=jnp.float32)
        + jnp.dot(theirs, w_other[...], preferred_element_type=jnp.float32)
    ).astype(jnp.bfloat16)

    for h in range(4):

        @pl.when(jnp.logical_not(ring * RING + 2 * h + home == me))
        def _():
            pltpu.make_async_remote_copy(
                src_ref=vg.at[0],
                dst_ref=vg_recv.at[h],
                send_sem=vg_send_sem.at[0],
                recv_sem=vg_sem.at[h],
                device_id=(partner, grp),
                device_id_type=MESH,
            ).wait_recv()

    vgrad_ref[...] = vg_recv[...].reshape(4 * HD, TOK).T

    for stream in (keys, vals, grads):
        stream.finish()
    for batch in range(2):
        w_copy(batch, 0, me).wait_send()
        w_copy(batch, 1, across).wait_send()
        w_relay(batch).wait_send()
    lse_copy(0, 0, partner).wait_send()

    @pl.when(gets)
    def _():
        lse_copy(1, 0, partner).wait_send()

    for b in range(4):
        att_copy(b, other).wait_send()

        @pl.when(jnp.logical_not(owner(b) == me))
        def _():
            att_copy(b, grp).wait_send()
            vg_copy(b).wait_send()


def store(mixed_vmem, vgrad_vmem, mixed_hbm, vgrad_hbm, sem):
    copies = [
        pltpu.make_async_copy(mixed_vmem, mixed_hbm, sem.at[0]),
        pltpu.make_async_copy(vgrad_vmem, vgrad_hbm, sem.at[1]),
    ]
    for copy in copies:
        copy.start()
    for copy in copies:
        copy.wait()


def shards(queries, values, scales, block_reach, out_weight, out_grad):
    vmem = pl.BlockSpec(memory_space=pltpu.VMEM)
    hbm = pl.BlockSpec(memory_space=pltpu.HBM)

    def in_hbm(array):
        return pltpu.with_memory_space_constraint(array, pltpu.HBM)

    bf16, f32 = jnp.bfloat16, jnp.float32
    dma = pltpu.SemaphoreType.DMA
    mixed, vgrad = pl.pallas_call(
        kernel,
        out_shape=(
            jax.ShapeDtypeStruct((TOK // 2, D), bf16),
            jax.ShapeDtypeStruct((TOK, HEADS_DEV * HD), bf16),
        ),
        in_specs=[hbm, hbm, hbm, hbm, pl.BlockSpec(memory_space=pltpu.SMEM), hbm],
        out_specs=(vmem, vmem),
        scratch_shapes=[
            pltpu.VMEM((TOK, HEADS_DEV * HD), bf16),
            pltpu.VMEM((TOK, HEADS_DEV * HD), bf16),
            pltpu.VMEM((TOK, HEADS_DEV * HD), bf16),
            pltpu.VMEM((HEADS_DEV, TOK), f32),
            pltpu.VMEM((HEADS_DEV * HD, D), bf16),
            pltpu.VMEM((4, ROWS, HALF), bf16),
            pltpu.VMEM((4, HD, TOK), bf16),
            pltpu.VMEM((4, HD, TOK), bf16),
            pltpu.VMEM((12, ROWS, HALF), bf16),
            pltpu.VMEM((12, HD, TOK), bf16),
            pltpu.VMEM((12, HD, TOK), bf16),
            pltpu.VMEM((12, TOK, HD), bf16),
            pltpu.VMEM((36, TOK, TOK), f32),
            pltpu.VMEM((36, TOK, TOK), bf16),
            pltpu.VMEM((12, TOK, 128), f32),
            pltpu.VMEM((36, 1, TOK), f32),
            pltpu.VMEM((4, 1, TOK), f32),
            pltpu.VMEM((4, 1, TOK), f32),
            pltpu.VMEM((4, HD, TOK), f32),
            pltpu.VMEM((3, 8, TOK), f32),
            pltpu.VMEM((4, HD, TOK), bf16),
            pltpu.VMEM((8, HD, TOK // 2), bf16),
            pltpu.VMEM((4, HD, TOK), bf16),
            pltpu.VMEM((4, HD, TOK), bf16),
            pltpu.VMEM((TOK, D), bf16),
            dma((12,)),
            dma((11,)),
            dma((12,)),
            dma((11,)),
            dma((12,)),
            dma((11,)),
            dma((3,)),
            dma((2,)),
            dma((8,)),
            dma((4, 2)),
            dma((4,)),
            dma((4,)),
            dma((6,)),
            dma((6,)),
            dma((5,)),
        ],
        compiler_params=pltpu.CompilerParams(
            collective_id=0, has_side_effects=True, vmem_limit_bytes=40 * 1024 * 1024
        ),
    )(
        in_hbm(queries),
        in_hbm(values),
        in_hbm(out_grad),
        in_hbm(scales.T),
        block_reach,
        in_hbm(out_weight),
    )
    return pl.pallas_call(
        store,
        out_shape=(
            jax.ShapeDtypeStruct((TOK // 2, D), bf16),
            jax.ShapeDtypeStruct((TOK, HEADS_DEV * HD), bf16),
        ),
        in_specs=[vmem, vmem],
        out_specs=(hbm, hbm),
        scratch_shapes=[dma((2,))],
    )(
        pltpu.with_memory_space_constraint(mixed, pltpu.VMEM),
        pltpu.with_memory_space_constraint(vgrad, pltpu.VMEM),
    )


def solution(mesh):
    return jax.shard_map(
        shards,
        mesh=mesh,
        in_specs=(
            P("seq", "head"),
            P("seq", "head"),
            P("seq", "head"),
            P("seq"),
            P("head", None),
            P("seq", "head"),
        ),
        out_specs=(P(("seq", "head"), None), P("seq", "head")),
        check_vma=False,
    )
```

```python
import jax
import jax.numpy as jnp
from jax import lax
from jax.experimental import pallas as pl
from jax.experimental.pallas import tpu as pltpu
from jax.sharding import PartitionSpec as P

HD = 64
TOK = 256
HEADS_DEV = 4
D = 1024
RINGS = 16
RING = 8
NBLK = 128
ROWS = 2 * HD + 16
HALF = TOK // 2
MESH = pl.DeviceIdType.MESH
START = -1e30
NEGATIVE = -1e30
BARRED = -3e30


def kernel(
    q_hbm,
    v_hbm,
    g_hbm,
    scale_hbm,
    reach_ref,
    w_hbm,
    mixed_ref,
    vgrad_ref,
    q_ref,
    v_ref,
    g_ref,
    scale_ref,
    w_ref,
    send,
    send_v,
    send_g,
    buf,
    buf_v,
    buf_g,
    kf,
    tiles,
    weights,
    columns,
    tile_tops,
    top,
    tot,
    acc,
    lse,
    att,
    att_recv,
    vg,
    vg_recv,
    w_other,
    slot_sem,
    send_sem,
    slot_v_sem,
    send_v_sem,
    slot_g_sem,
    send_g_sem,
    lse_sem,
    lse_send_sem,
    att_sem,
    att_send_sem,
    vg_sem,
    vg_send_sem,
    w_sem,
    w_send_sem,
    in_sem,
):
    me = lax.axis_index("seq")
    grp = lax.axis_index("head")
    ring = me // RING
    inner = me % RING
    y = inner // 2
    k = inner % 2
    other = 1 - grp
    home = y // 2
    partner = me + 1 - 2 * k
    prev_ring = ((ring + RINGS - 1) % RINGS) * RING
    next_ring = ((ring + 1) % RINGS) * RING
    up = y // 2
    across = me + RING - 2 * RING * (ring % 2)

    halo_from = prev_ring * (1 - k) + next_ring * k + 4 * (1 - k)
    lse_peer = (prev_ring + 2 * y + 1) * (1 - k) + (next_ring + 2 * y) * k
    halo_to = (next_ring) * up + (prev_ring + 1) * (1 - up)
    halo_slot = (2 * y + k - 4) * up + (2 * y + k + 8) * (1 - up)
    own_slot = 2 * y + 4 - 3 * k
    partner_slot = 2 * y + 5 * k
    is_home = (home == k).astype(jnp.int32)
    first, last = ring == 0, ring == RINGS - 1
    gets = jnp.logical_not(jnp.logical_or(jnp.logical_and(first, k == 0), jnp.logical_and(last, k == 1)))
    gives = jnp.logical_not(jnp.logical_or(jnp.logical_and(first, up == 0), jnp.logical_and(last, up == 1)))
    expected = 14 - is_home + gets.astype(jnp.int32) + 4 * gives.astype(jnp.int32)

    barrier = pltpu.get_barrier_semaphore()
    loads = [
        pltpu.make_async_copy(source, target, in_sem.at[i])
        for i, (source, target) in enumerate(
            (
                (q_hbm, q_ref),
                (scale_hbm, scale_ref),
                (v_hbm, v_ref),
                (g_hbm, g_ref),
                (w_hbm, w_ref),
            )
        )
    ]
    for load in loads:
        load.start()

    def greet(seq, head):
        pl.semaphore_signal(barrier, inc=1, device_id=(seq, head), device_id_type=MESH)

    greet(partner, grp)
    for step in range(1, 4):
        greet(ring * RING + 2 * ((y + step) % 4) + k, grp)

    @pl.when(gets)
    def _():
        for j in range(4):
            greet(halo_from + j, grp)
        greet(lse_peer, grp)

    for h in range(4):
        source = ring * RING + 2 * h + home
        greet(source, other)

        @pl.when(jnp.logical_not(source == me))
        def _():
            greet(source, grp)

    greet(me, other)
    greet(across, other)

    for load in loads[:2]:
        load.wait()
    q_t = q_ref[...].T
    reach_rows = jnp.full((16, HALF), reach_ref[0].astype(jnp.float32)).astype(jnp.bfloat16)
    for h in range(HEADS_DEV):
        part = q_t[h * HD : (h + 1) * HD, :].astype(jnp.float32)
        square = jnp.sum(part * part, axis=0, keepdims=True)
        direction = part * lax.rsqrt(square + 1e-06)
        key = (direction * scale_ref[h : h + 1, :]).astype(jnp.bfloat16)
        send[h, 0:HD, :] = key[:, 0:HALF]
        send[h, HD : 2 * HD, :] = key[:, HALF:]
        send[h, 2 * HD :, :] = reach_rows

    pl.semaphore_wait(barrier, expected)

    class Stream:
        def __init__(self, source, place, arrive, sent):
            self.source, self.place, self.arrive, self.sent = source, place, arrive, sent

        def copy(self, src, slot, which, seq):
            return pltpu.make_async_remote_copy(
                src_ref=src,
                dst_ref=self.place.at[slot],
                send_sem=self.sent.at[which],
                recv_sem=self.arrive.at[slot],
                device_id=(seq, grp),
                device_id_type=MESH,
            )

        def start(self):
            for step in (2, 1, 3):
                target = (y + step) % 4
                self.copy(
                    self.source.at[target], own_slot, step, ring * RING + 2 * target + k
                ).start()
            self.copy(self.source.at[y], partner_slot, 0, partner).start()

            @pl.when(gives)
            def _():
                for step in (0, 1, 3, 2):
                    target = (y + step) % 4
                    self.copy(
                        self.source.at[target], halo_slot, 4 + step, halo_to + 2 * target
                    ).start()

        def arrived(self, slot):
            self.copy(self.source.at[0], slot, 0, partner).wait_recv()

        def relay(self, use=None):
            for step in (1, 3, 2):
                source = (y + step) % 4
                slot = 2 * source + 4 - 3 * k
                self.arrived(slot)
                self.copy(self.place.at[slot], 2 * source + 5 * k, 7 + step, partner).start()
                if use is not None:
                    use(slot)

        def ring_arrived(self, use=None):
            for step in (0, 1, 3, 2):
                slot = 2 * ((y + step) % 4) + 5 - 5 * k
                self.arrived(slot)
                if use is not None:
                    use(slot)

        def halo_arrived(self):
            @pl.when(gets)
            def _():
                for m in range(4):
                    self.arrived((8 + m) * k + (3 - m) * (1 - k))

        def finish(self):
            for which in (0, 1, 2, 3, 8, 9, 10):
                self.copy(self.source.at[0], 0, which, partner).wait_send()

            @pl.when(gives)
            def _():
                for which in range(4, 8):
                    self.copy(self.source.at[0], 0, which, partner).wait_send()

    keys = Stream(send, buf, slot_sem, send_sem)
    vals = Stream(send_v, buf_v, slot_v_sem, send_v_sem)
    grads = Stream(send_g, buf_g, slot_g_sem, send_g_sem)
    keys.start()
    for load in loads[2:4]:
        load.wait()
    v_t = v_ref[...].T
    g_t = g_ref[...].T
    for h in range(HEADS_DEV):
        send_v[h] = v_t[h * HD : (h + 1) * HD, :]
        send_g[h] = g_t[h * HD : (h + 1) * HD, :]
    buf[own_slot] = send[y]
    buf_v[own_slot] = send_v[y]
    buf_g[own_slot] = send_g[y]

    @pl.when(jnp.logical_not(gets))
    def _():
        for m in range(4):
            slot = (8 + m) * k + m * (1 - k)
            buf[slot] = jnp.zeros((ROWS, HALF), jnp.bfloat16)
            buf_v[slot] = jnp.zeros((HD, TOK), jnp.bfloat16)
            buf_g[slot] = jnp.zeros((HD, TOK), jnp.bfloat16)
        lse[2 * k] = jnp.zeros((8, TOK), jnp.float32)

    vals.start()
    grads.start()

    def key_of(slot):
        return jnp.concatenate([buf[slot, 0:HD, :], buf[slot, HD : 2 * HD, :]], axis=1)

    def turn(slot):
        kf[slot] = key_of(slot).T

    turn(own_slot)
    keys.relay(turn)
    keys.ring_arrived(turn)

    first_block = ring * RING + 4 * k - 4

    def allowed_row(slot, b, distance):
        index = first_block + slot
        valid = jnp.logical_and(index >= 0, index < NBLK)
        needed = jnp.where(valid, distance, 99).astype(jnp.float32)
        far = buf[slot, 2 * HD :, :].astype(jnp.float32)[0:1]
        mine = buf[4 + b, 2 * HD :, :].astype(jnp.float32)[0:1]
        row = needed <= jnp.minimum(far, mine)
        return jnp.concatenate([row, row], axis=1)

    def score_tile(tile):
        slot, b, place, distance = tile
        scores = jnp.dot(kf[slot], key_of(4 + b), preferred_element_type=jnp.float32)
        if distance is None:
            row = lax.broadcasted_iota(jnp.int32, (TOK, TOK), 0)
            column = lax.broadcasted_iota(jnp.int32, (TOK, TOK), 1)
            scores = jnp.where(row == column, NEGATIVE, scores)
        tiles[place] = scores

    def exponent_tile(tile):
        slot, b, place, distance = tile
        scores = tiles[place]
        tile_top = jnp.max(scores, axis=0, keepdims=True)
        exponent = jnp.exp(scores - tile_top)
        weights[place] = exponent.astype(jnp.bfloat16)
        tile_sum = jnp.sum(exponent, axis=0, keepdims=True)
        if distance is None:
            tile_tops[place], top[b], tot[b] = tile_top, tile_top, tile_sum
            return
        tile_top = jnp.where(allowed_row(slot, b, distance), tile_top, BARRED)
        new_top = jnp.maximum(top[b], tile_top)
        tile_tops[place] = tile_top
        tot[b] = jnp.exp(top[b] - new_top) * tot[b] + jnp.exp(tile_top - new_top) * tile_sum
        top[b] = new_top

    def exponents(work):
        for t in range(len(work) + 2):
            if t >= 2:
                exponent_tile(work[t - 2])
            if t < len(work):
                score_tile(work[t])

    def numerator_tile(tile):
        slot, b, place, _ = tile
        part = jnp.dot(buf_v[slot], weights[place], preferred_element_type=jnp.float32)
        return jnp.exp(tile_tops[place] - top[b]) * part

    square = [
        (4 + i, (i + step) % 4, 9 * ((i + step) % 4) + 4 + i - (i + step) % 4, abs(i - (i + step) % 4) or None)
        for step in range(4)
        for i in range(4)
    ]

    def side(right):
        work = []
        for q in range(4):
            for m in range(q + 1):
                slot = (8 + m) * right + (3 - m) * (1 - right)
                b = q * right + (3 - q) * (1 - right)
                work.append((slot, b, 9 * b + slot - b, 4 + m - q))
        return work

    near, far = 1 - k, k

    exponents(square + side(near))
    vals.relay()
    loads[4].wait()
    def w_copy(batch, which, seq):
        rows = pl.ds(pl.multiple_of(k * 128 + batch * 64 + which * 32, 32), 32)
        return pltpu.make_async_remote_copy(
            src_ref=w_ref.at[rows],
            dst_ref=w_other.at[rows],
            send_sem=w_send_sem.at[2 * batch + which],
            recv_sem=w_sem.at[2 * batch + which],
            device_id=(seq, other),
            device_id_type=MESH,
        )

    def w_relay(batch):
        rows = pl.ds(pl.multiple_of(k * 128 + batch * 64, 64), 64)
        return pltpu.make_async_remote_copy(
            src_ref=w_other.at[rows],
            dst_ref=w_other.at[rows],
            send_sem=w_send_sem.at[4 + batch],
            recv_sem=w_sem.at[4 + batch],
            device_id=(partner, grp),
            device_id_type=MESH,
        )

    def send_w(batch):
        w_copy(batch, 0, me).start()
        w_copy(batch, 1, across).start()

    def pass_w(batch):
        w_copy(batch, 0, me).wait_recv()
        w_copy(batch, 1, across).wait_recv()
        w_relay(batch).start()

    send_w(0)
    keys.halo_arrived()
    for m in range(4):
        turn((8 + m) * far + (3 - m) * (1 - far))
    exponents(side(far))

    denominators = [top[b] + jnp.log(tot[b]) for b in range(4)]
    lse[1] = jnp.concatenate(denominators + denominators, axis=0)

    def lse_copy(which, place, seq):
        return pltpu.make_async_remote_copy(
            src_ref=lse.at[1],
            dst_ref=lse.at[place],
            send_sem=lse_send_sem.at[which],
            recv_sem=lse_sem.at[place],
            device_id=(seq, grp),
            device_id_type=MESH,
        )

    @pl.when(gets)
    def _():
        lse_copy(1, 2 * (1 - k), lse_peer).start()

    lse_copy(0, 2 * k, partner).start()
    send_w(1)

    grads.relay()
    vals.ring_arrived()
    for b in range(4):
        total = None
        for tile in square:
            if tile[1] == b:
                part = numerator_tile(tile)
                total = part if total is None else total + part
        acc[b] = total

    def add_side(right, tile_of):
        work = side(right)
        for q in (3, 2, 1, 0):
            first = q * (q + 1) // 2
            b = work[first][1]
            total = acc[b]
            for tile in work[first : first + q + 1]:
                total = total + tile_of(tile)
            acc[b] = total

    add_side(near, numerator_tile)
    vals.halo_arrived()
    add_side(far, numerator_tile)
    for b in range(4):
        att[b] = (acc[b] * (1.0 / tot[b])).astype(jnp.bfloat16)

    def att_copy(b, head):
        return pltpu.make_async_remote_copy(
            src_ref=att.at[b, :, pl.ds(pl.multiple_of(head * 128, 128), 128)],
            dst_ref=att_recv.at[grp * 4 + y],
            send_sem=att_send_sem.at[b, head],
            recv_sem=att_sem.at[grp * 4 + y],
            device_id=(ring * RING + 4 * k + b, head),
            device_id_type=MESH,
        )

    def owner(b):
        return ring * RING + 4 * k + b

    for b in range(4):
        att_copy(b, other).start()

        @pl.when(jnp.logical_not(owner(b) == me))
        def _():
            att_copy(b, grp).start()

    @pl.when(home == k)
    def _():
        b = inner - 4 * k
        att_recv[grp * 4 + y] = att[b, :, pl.ds(pl.multiple_of(grp * 128, 128), 128)]

    def turn_lse(place):
        for row in range(4):
            value = jnp.broadcast_to(lse[place, pl.ds(row, 1), :], (128, TOK))
            columns[4 * place + row] = value.T

    def backward_tile(tile):
        slot, b, place, distance = tile
        column = columns[slot]
        shifted = tiles[place] - jnp.concatenate([column, column], axis=1)
        share = jnp.exp(shifted).astype(jnp.bfloat16)
        part = jnp.dot(buf_g[slot], share, preferred_element_type=jnp.float32)
        if distance is None:
            return part
        return jnp.where(allowed_row(slot, b, distance), part, 0.0)

    grads.ring_arrived()
    turn_lse(1)
    for b in range(4):
        total = None
        for tile in square:
            if tile[1] == b:
                part = backward_tile(tile)
                total = part if total is None else total + part
        acc[b] = total

    lse_copy(0, 2 * near, partner).wait_recv()
    turn_lse(2 * near)
    add_side(near, backward_tile)
    @pl.when(gets)
    def _():
        lse_copy(0, 2 * far, partner).wait_recv()

    grads.halo_arrived()
    turn_lse(2 * far)
    add_side(far, backward_tile)

    for b in range(4):
        vg[b] = acc[b].astype(jnp.bfloat16)

    def vg_copy(b):
        return pltpu.make_async_remote_copy(
            src_ref=vg.at[b],
            dst_ref=vg_recv.at[y],
            send_sem=vg_send_sem.at[b],
            recv_sem=vg_sem.at[y],
            device_id=(owner(b), grp),
            device_id_type=MESH,
        )

    for b in range(4):

        @pl.when(jnp.logical_not(owner(b) == me))
        def _():
            vg_copy(b).start()

    @pl.when(home == k)
    def _():
        vg_recv[y] = vg[inner - 4 * k]

    pass_w(0)
    pass_w(1)

    def att_arrived(place):
        pltpu.make_async_remote_copy(
            src_ref=att.at[0, :, pl.ds(0, 128)],
            dst_ref=att_recv.at[place],
            send_sem=att_send_sem.at[0, 0],
            recv_sem=att_sem.at[place],
            device_id=(me, other),
            device_id_type=MESH,
        ).wait_recv()

    for h in range(4):
        att_arrived(other * 4 + h)

        @pl.when(jnp.logical_not(ring * RING + 2 * h + home == me))
        def _():
            att_arrived(grp * 4 + h)

    w_relay(0).wait_recv()
    w_relay(1).wait_recv()
    mine = att_recv[pl.ds(grp * 4, 4)].reshape(4 * HD, 128).T
    theirs = att_recv[pl.ds(other * 4, 4)].reshape(4 * HD, 128).T
    mixed_ref[...] = (
        jnp.dot(mine, w_ref[...], preferred_element_type=jnp.float32)
        + jnp.dot(theirs, w_other[...], preferred_element_type=jnp.float32)
    ).astype(jnp.bfloat16)

    for h in range(4):

        @pl.when(jnp.logical_not(ring * RING + 2 * h + home == me))
        def _():
            pltpu.make_async_remote_copy(
                src_ref=vg.at[0],
                dst_ref=vg_recv.at[h],
                send_sem=vg_send_sem.at[0],
                recv_sem=vg_sem.at[h],
                device_id=(partner, grp),
                device_id_type=MESH,
            ).wait_recv()

    vgrad_ref[...] = vg_recv[...].reshape(4 * HD, TOK).T

    for stream in (keys, vals, grads):
        stream.finish()
    for batch in range(2):
        w_copy(batch, 0, me).wait_send()
        w_copy(batch, 1, across).wait_send()
        w_relay(batch).wait_send()
    lse_copy(0, 0, partner).wait_send()

    @pl.when(gets)
    def _():
        lse_copy(1, 0, partner).wait_send()

    for b in range(4):
        att_copy(b, other).wait_send()

        @pl.when(jnp.logical_not(owner(b) == me))
        def _():
            att_copy(b, grp).wait_send()
            vg_copy(b).wait_send()


def store(mixed_vmem, vgrad_vmem, mixed_hbm, vgrad_hbm, sem):
    copies = [
        pltpu.make_async_copy(mixed_vmem, mixed_hbm, sem.at[0]),
        pltpu.make_async_copy(vgrad_vmem, vgrad_hbm, sem.at[1]),
    ]
    for copy in copies:
        copy.start()
    for copy in copies:
        copy.wait()


def shards(queries, values, scales, block_reach, out_weight, out_grad):
    vmem = pl.BlockSpec(memory_space=pltpu.VMEM)
    hbm = pl.BlockSpec(memory_space=pltpu.HBM)

    def in_hbm(array):
        return pltpu.with_memory_space_constraint(array, pltpu.HBM)

    bf16, f32 = jnp.bfloat16, jnp.float32
    dma = pltpu.SemaphoreType.DMA
    mixed, vgrad = pl.pallas_call(
        kernel,
        out_shape=(
            jax.ShapeDtypeStruct((TOK // 2, D), bf16),
            jax.ShapeDtypeStruct((TOK, HEADS_DEV * HD), bf16),
        ),
        in_specs=[hbm, hbm, hbm, hbm, pl.BlockSpec(memory_space=pltpu.SMEM), hbm],
        out_specs=(vmem, vmem),
        scratch_shapes=[
            pltpu.VMEM((TOK, HEADS_DEV * HD), bf16),
            pltpu.VMEM((TOK, HEADS_DEV * HD), bf16),
            pltpu.VMEM((TOK, HEADS_DEV * HD), bf16),
            pltpu.VMEM((HEADS_DEV, TOK), f32),
            pltpu.VMEM((HEADS_DEV * HD, D), bf16),
            pltpu.VMEM((4, ROWS, HALF), bf16),
            pltpu.VMEM((4, HD, TOK), bf16),
            pltpu.VMEM((4, HD, TOK), bf16),
            pltpu.VMEM((12, ROWS, HALF), bf16),
            pltpu.VMEM((12, HD, TOK), bf16),
            pltpu.VMEM((12, HD, TOK), bf16),
            pltpu.VMEM((12, TOK, HD), bf16),
            pltpu.VMEM((36, TOK, TOK), f32),
            pltpu.VMEM((36, TOK, TOK), bf16),
            pltpu.VMEM((12, TOK, 128), f32),
            pltpu.VMEM((36, 1, TOK), f32),
            pltpu.VMEM((4, 1, TOK), f32),
            pltpu.VMEM((4, 1, TOK), f32),
            pltpu.VMEM((4, HD, TOK), f32),
            pltpu.VMEM((3, 8, TOK), f32),
            pltpu.VMEM((4, HD, TOK), bf16),
            pltpu.VMEM((8, HD, TOK // 2), bf16),
            pltpu.VMEM((4, HD, TOK), bf16),
            pltpu.VMEM((4, HD, TOK), bf16),
            pltpu.VMEM((TOK, D), bf16),
            dma((12,)),
            dma((11,)),
            dma((12,)),
            dma((11,)),
            dma((12,)),
            dma((11,)),
            dma((3,)),
            dma((2,)),
            dma((8,)),
            dma((4, 2)),
            dma((4,)),
            dma((4,)),
            dma((6,)),
            dma((6,)),
            dma((5,)),
        ],
        compiler_params=pltpu.CompilerParams(
            collective_id=0, has_side_effects=True, vmem_limit_bytes=40 * 1024 * 1024
        ),
    )(
        in_hbm(queries),
        in_hbm(values),
        in_hbm(out_grad),
        in_hbm(scales.T),
        block_reach,
        in_hbm(out_weight),
    )
    return pl.pallas_call(
        store,
        out_shape=(
            jax.ShapeDtypeStruct((TOK // 2, D), bf16),
            jax.ShapeDtypeStruct((TOK, HEADS_DEV * HD), bf16),
        ),
        in_specs=[vmem, vmem],
        out_specs=(hbm, hbm),
        scratch_shapes=[dma((2,))],
    )(
        pltpu.with_memory_space_constraint(mixed, pltpu.VMEM),
        pltpu.with_memory_space_constraint(vgrad, pltpu.VMEM),
    )


def solution(mesh):
    return jax.shard_map(
        shards,
        mesh=mesh,
        in_specs=(
            P("seq", "head"),
            P("seq", "head"),
            P("seq", "head"),
            P("seq"),
            P("head", None),
            P("seq", "head"),
        ),
        out_specs=(P(("seq", "head"), None), P("seq", "head")),
        check_vma=False,
    )
```
